128 devices in a mesh: batch: 1, group: 128 (over z, y, x, core).
Axes of the slice: x: 4, y: 4, z: 4, core: 2. Of those that a mesh axis runs over, the one named last changes fastest.
Arguments:
- sort_keys: float32 [65536], P(('batch', 'group'))
- seg_ids: int32 [65536], P(('batch', 'group'))
- payload: bfloat16 [65536, 2048], P(('batch', 'group'))
Outputs:
- output: bfloat16 [65536, 2048], P(('batch', 'group'))
All inputs are finite; a program needn't handle non-finite values.
Results may differ from the reference program's by a relative error of at most 0.00688365.
Values are sent between devices in bfloat16 or wider.
A program may use at most 1 GiB of HBM per device.

```python
import jax
import jax.numpy as jnp
from jax import lax

GROUP = 128
ROWS_DEV = 512
WIDTH = 2048
TOTAL = GROUP * ROWS_DEV
PAIR = ROWS_DEV // GROUP


def combine_runs(left_part, right_part):
    left_flag, left_rows = left_part
    right_flag, right_rows = right_part
    joined = jnp.where(right_flag[..., None], right_rows, left_rows + right_rows)
    return jnp.logical_or(left_flag, right_flag), joined


def draw_layout(base_key):
    phase_key, size_key, tie_key, place_key, cut_key, base_id_key = jax.random.split(base_key, 6)
    half_pair = PAIR // 2
    dev_phase = jax.random.permutation(phase_key, GROUP)
    bound_no = jnp.arange(1, GROUP, dtype=jnp.int32)
    bound_phase = (dev_phase[:, None] + bound_no[None, :]) % GROUP
    shift_size = jax.random.randint(size_key, (GROUP, GROUP - 1), 0, half_pair + 1)
    cut_shift = jnp.where(bound_phase < GROUP // 2, jnp.maximum(shift_size, 1), -shift_size)
    cut_shift = jnp.where(bound_phase == GROUP // 2, 0, cut_shift)
    full_dev = dev_phase == GROUP - 2
    cut_shift = cut_shift.at[:, 0].set(jnp.where(full_dev, -half_pair, cut_shift[:, 0]))
    cut_shift = cut_shift.at[:, 1].set(jnp.where(full_dev, half_pair, cut_shift[:, 1]))
    band_cuts = bound_no[None, :] * PAIR + cut_shift
    local_rank = jnp.arange(ROWS_DEV, dtype=jnp.int32)

    def band_search(cut_row):
        return jnp.searchsorted(cut_row, local_rank, side='right')

    band_of = jax.vmap(band_search)(band_cuts).astype(jnp.int32)
    prev_band = jnp.maximum(band_of - 1, 0)
    band_low = jnp.take_along_axis(band_cuts, prev_band, axis=1)
    band_phase = jnp.take_along_axis(bound_phase, prev_band, axis=1)
    lead_row = (band_of >= 1) & (local_rank[None, :] == band_low) & (band_phase == GROUP // 2)
    tie_break = jax.random.permutation(tie_key, TOTAL).reshape(GROUP, ROWS_DEV)
    rank_score = band_of * (TOTAL + 1) + jnp.where(lead_row, 0, tie_break + 1)
    score_order = jnp.argsort(rank_score.reshape(-1), stable=True)
    global_rank = jnp.argsort(score_order, stable=True).astype(jnp.int32).reshape(GROUP, ROWS_DEV)
    place_keys = jax.random.split(place_key, GROUP)

    def place_rows(row_key):
        return jax.random.permutation(row_key, ROWS_DEV)

    placement = jax.vmap(place_rows)(place_keys)
    rank_at = jnp.take_along_axis(global_rank, placement, axis=1).reshape(TOTAL)
    seg_cuts = jnp.sort(jax.random.randint(cut_key, (GROUP - 1,), 1, TOTAL))
    first_id = jax.random.randint(base_id_key, (), 0, 1000)
    seg_ids = (jnp.searchsorted(seg_cuts, rank_at, side='right') + first_id).astype(jnp.int32)
    return rank_at, seg_ids


def setup_inputs(seed: int = 0, part: int = 0) -> dict:
    base_key = jax.random.fold_in(jax.random.key(seed), part)
    layout_key, payload_key = jax.random.split(base_key, 2)
    rank_at, seg_ids = draw_layout(layout_key)
    centred = (2 * rank_at + 1 - TOTAL).astype(jnp.float32) / TOTAL
    sort_keys = centred * centred * centred
    noise = jax.random.normal(payload_key, (TOTAL, WIDTH), jnp.float32)
    payload = (noise * ROWS_DEV ** -0.5).astype(jnp.bfloat16)
    return {'sort_keys': sort_keys, 'seg_ids': seg_ids, 'payload': payload}


def reference(sort_keys, seg_ids, payload):
    row_pos = jnp.arange(sort_keys.shape[0], dtype=jnp.int32)
    _, seg_sorted, sort_order = lax.sort((sort_keys, seg_ids, row_pos), num_keys=1)
    run_rows = payload[sort_order].astype(jnp.float32)
    first_flag = jnp.ones((1,), dtype=jnp.bool_)
    run_start = jnp.concatenate([first_flag, seg_sorted[1:] != seg_sorted[:-1]])
    _, scanned = lax.associative_scan(combine_runs, (run_start, run_rows))
    _, back_order = lax.sort((sort_order, row_pos), num_keys=1)
    return scanned[back_order].astype(jnp.bfloat16)
```

```python
import functools

import jax
import jax.numpy as jnp
from jax import lax
from jax.experimental import pallas as pl
from jax.experimental.pallas import tpu as pltpu
from jax.sharding import PartitionSpec as P

F32 = jnp.float32
BF16 = jnp.bfloat16
I32 = jnp.int32
NEG = float('-inf')
POS = float('inf')

DEVS = 128
ROWS = 512
WIDTH = 2048
SPLIT = 2
CAP = 8 * SPLIT
GROUPS = DEVS // SPLIT
COLS = WIDTH // SPLIT
PACK = GROUPS * CAP
SLOTS = DEVS * CAP
TAILW = COLS + 128


def iota(shape, dim):
    return lax.broadcasted_iota(I32, shape, dim)


def peer(me, idx):
    core, x, y, z = me % 2, (me // 2) % 4, (me // 8) % 4, me // 32
    blk, turn, flip = idx // 8, (idx // 2) % 4, idx % 2
    dst_x = (x + turn) % 4
    dst_y = (y + turn + blk % 4) % 4
    dst_z = (z + turn + blk // 4) % 4
    return ((dst_z * 4 + dst_y) * 4 + dst_x) * 2 + (core + flip) % 2


def kernel(keys_ref, segs_ref, pay_ref, out_ref, samp_msg, samp_all, packed, recv, meta_msg, meta_all, mask_ref,
           kcol_ref, scol_ref, bcol_ref, krow_ref, srow_ref, tail_msg, tail_all, sums_ref, ret, send_sem, samp_sem,
           meta_sem, row_sem, tail_sem, ret_sem):
    me = lax.axis_index('group')
    my_group = me // SPLIT
    my_part = me % SPLIT
    barrier = pltpu.get_barrier_semaphore()

    def remote(src, dst, recv_sem, dev):
        return pltpu.make_async_remote_copy(src_ref=src, dst_ref=dst, send_sem=send_sem, recv_sem=recv_sem,
                                            device_id={'group': dev}, device_id_type=pl.DeviceIdType.MESH)

    def each_peer(fn):
        def step(idx, carry):
            fn(peer(me, idx))
            return carry
        lax.fori_loop(1, DEVS, step, 0)

    each_peer(lambda dev: pl.semaphore_signal(barrier, inc=1, device_id={'group': dev},
                                              device_id_type=pl.DeviceIdType.MESH))

    key_row = keys_ref[...]
    seg_row = segs_ref[...]
    eye = iota((ROWS, ROWS), 0) == iota((ROWS, ROWS), 1)

    def to_col(row):
        return jnp.sum(jnp.where(eye, jnp.broadcast_to(row, (ROWS, ROWS)), 0), axis=1, keepdims=True)

    def to_row(col):
        return jnp.sum(jnp.where(eye, jnp.broadcast_to(col, (ROWS, ROWS)), 0), axis=0, keepdims=True)

    key_col = to_col(key_row)
    rank_col = jnp.sum(jnp.where(key_row < key_col, 1.0, 0.0), axis=1, keepdims=True)
    quad = iota((ROWS, DEVS), 1).astype(F32) * 4.0
    samp_msg[...] = jnp.sum(jnp.where(rank_col == quad, jnp.broadcast_to(key_col, (ROWS, DEVS)), 0.0), axis=0,
                            keepdims=True)
    pl.semaphore_wait(barrier, DEVS - 1)

    each_peer(lambda dev: remote(samp_msg, samp_all.at[me], samp_sem, dev).start())
    samp_all[me] = samp_msg[...]
    remote(samp_all.at[pl.ds(0, DEVS - 1)], samp_all.at[pl.ds(0, DEVS - 1)], samp_sem, me).wait_recv()

    counts = []
    for part in range(ROWS // 128):
        kblk = jnp.broadcast_to(key_col[part * 128:(part + 1) * 128], (128, 128))

        def count(step, acc, kblk=kblk):
            for sub in range(8):
                acc = acc + jnp.where(samp_all[step * 8 + sub] <= kblk, 1.0, 0.0)
            return acc

        acc = lax.fori_loop(0, DEVS // 8, count, jnp.zeros((128, 128), F32))
        counts.append(jnp.sum(acc, axis=1, keepdims=True))
    seen_col = jnp.concatenate(counts, axis=0)
    group_col = jnp.maximum(jnp.floor((seen_col - (DEVS // 2 + 1)) * (1.0 / (DEVS * SPLIT))), 0.0)
    group_row = to_row(group_col)
    slot_col = rank_col - jnp.sum(jnp.where(group_row < group_col, 1.0, 0.0), axis=1, keepdims=True)
    place_col = group_col * CAP + slot_col
    place_row = to_row(place_col)

    hi_row = (seg_row // 65536).astype(F32)
    lo_row = (seg_row % 65536).astype(F32)
    pack_blk = 256

    def pack(step, carry):
        base = step * pack_blk
        hit = place_row == (iota((pack_blk, ROWS), 0) + base).astype(F32)
        slot = iota((pack_blk, 128), 0) % CAP
        lane = iota((pack_blk, 128), 1)
        spread = jnp.zeros((pack_blk, 128), F32)
        for no, val in enumerate((key_row, hi_row, lo_row, jnp.ones((1, ROWS), F32))):
            got = jnp.sum(jnp.where(hit, jnp.broadcast_to(val, (pack_blk, ROWS)), 0.0), axis=1, keepdims=True)
            spread = spread + jnp.where(lane == slot + no * CAP, got, 0.0)
        meta = jnp.sum(spread.reshape(pack_blk // CAP, CAP, 128), axis=1, keepdims=True)
        meta_msg[pl.ds(step * (pack_blk // CAP), pack_blk // CAP)] = meta
        hot = jnp.where(hit, 1.0, 0.0).astype(BF16)
        for part in range(SPLIT):
            rows = jnp.dot(hot, pay_ref[:, part * COLS:(part + 1) * COLS], preferred_element_type=F32)
            packed[part, pl.ds(pl.multiple_of(base, pack_blk), pack_blk)] = rows.astype(BF16)
        return carry

    lax.fori_loop(0, PACK // pack_blk, pack, 0)

    def my_rows(dev):
        return pl.ds(pl.multiple_of(dev * CAP, CAP), CAP)

    each_peer(lambda dev: remote(meta_msg.at[dev // SPLIT], meta_all.at[me], meta_sem, dev).start())
    each_peer(lambda dev: remote(packed.at[dev % SPLIT, my_rows(dev // SPLIT)], recv.at[my_rows(me)], row_sem, dev).start())
    meta_all[me] = meta_msg[my_group]
    recv[my_rows(me)] = packed[my_part, my_rows(my_group)]
    remote(meta_all.at[pl.ds(0, DEVS - 1)], meta_all.at[pl.ds(0, DEVS - 1)], meta_sem, me).wait_recv()

    col_blk = 128

    def columns(step, carry):
        got = meta_all[pl.ds(step * (col_blk // CAP), col_blk // CAP)]
        got = jnp.broadcast_to(got, (col_blk // CAP, CAP, 128)).reshape(col_blk, 128)
        slot = iota((col_blk, 128), 0) % CAP
        lane = iota((col_blk, 128), 1)
        vals = [jnp.sum(jnp.where(lane == slot + no * CAP, got, 0.0), axis=1, keepdims=True) for no in range(4)]
        live = vals[3] > 0.0
        seg = vals[1].astype(I32) * 65536 + vals[2].astype(I32)
        rows = pl.ds(pl.multiple_of(step * col_blk, col_blk), col_blk)
        kcol_ref[rows] = jnp.broadcast_to(jnp.where(live, vals[0], NEG), (col_blk, 128))
        scol_ref[rows] = jnp.broadcast_to(seg, (col_blk, 128))
        diag = iota((col_blk, 128), 0) == lane
        krow_ref[step] = jnp.sum(jnp.where(diag, jnp.where(live, vals[0], POS), 0.0), axis=0, keepdims=True)
        srow_ref[step] = jnp.sum(jnp.where(diag, seg, 0), axis=0, keepdims=True)
        return carry

    lax.fori_loop(0, SLOTS // col_blk, columns, 0)
    tiles = SLOTS // 128
    krow = [krow_ref[t] for t in range(tiles)]
    srow = [srow_ref[t] for t in range(tiles)]

    def masks(step, carry):
        rows = my_rows(step)
        kcol = kcol_ref[rows]
        scol = scol_ref[rows]
        best = jnp.full((CAP, 128), NEG, F32)
        for t in range(tiles):
            best = jnp.maximum(best, jnp.where((krow[t] < kcol) & (srow[t] != scol), krow[t], NEG))
        bound = jnp.broadcast_to(jnp.max(best, axis=1, keepdims=True), (CAP, 128))
        bcol_ref[rows] = bound
        for t in range(tiles):
            take = (krow[t] > bound) & (krow[t] <= kcol)
            mask_ref[rows, t * 128:(t + 1) * 128] = jnp.where(take, 1.0, 0.0).astype(BF16)
        return carry

    lax.fori_loop(0, DEVS, masks, 0)

    def over(vals, fold, red):
        acc = vals[0]
        for val in vals[1:]:
            acc = fold(acc, val)
        return red(acc, axis=1, keepdims=True)

    live_max = [jnp.where(k < POS, k, NEG) for k in krow]
    key_last = over(live_max, jnp.maximum, jnp.max)
    key_first = over(krow, jnp.minimum, jnp.min)
    hi_of = [(s // 65536).astype(F32) for s in srow]
    lo_of = [(s % 65536).astype(F32) for s in srow]

    def pick(key, vals):
        return over([jnp.where(k == key, v, 0.0) for k, v in zip(krow, vals)], jnp.add, jnp.sum)

    last_hi, last_lo = pick(key_last, hi_of), pick(key_last, lo_of)
    first_hi, first_lo = pick(key_first, hi_of), pick(key_first, lo_of)
    cut = over([jnp.where((k < POS) & ((h != last_hi) | (l != last_lo)), k, NEG)
                for k, h, l in zip(krow, hi_of, lo_of)], jnp.maximum, jnp.max)
    tail_hot = jnp.concatenate([jnp.where((k > cut) & (k < POS), 1.0, 0.0) for k in krow], axis=1)
    tail_hot = jnp.broadcast_to(tail_hot, (16, SLOTS)).astype(BF16)
    lane = iota((1, 128), 1)
    facts = jnp.zeros((1, 128), F32)
    for no, val in enumerate((first_hi, first_lo, last_hi, last_lo, jnp.where(cut > NEG, 1.0, 0.0))):
        facts = jnp.where(lane == no, val, facts)

    remote(recv.at[pl.ds(0, SLOTS - CAP)], recv.at[pl.ds(0, SLOTS - CAP)], row_sem, me).wait_recv()
    tail = jnp.dot(tail_hot, recv[...], preferred_element_type=F32)[0:1]
    tail_msg[:, :COLS] = tail
    tail_msg[:, COLS:] = facts

    def send_tail(step, carry):
        dst_group = (my_group + step) % GROUPS
        remote(tail_msg, tail_all.at[my_group], tail_sem, dst_group * SPLIT + my_part).start()
        return carry

    lax.fori_loop(1, GROUPS, send_tail, 0)
    tail_all[my_group] = tail_msg[...]
    remote(tail_all.at[pl.ds(0, GROUPS - 1)], tail_all.at[pl.ds(0, GROUPS - 1)], tail_sem, me).wait_recv()

    all_facts = tail_all[:, 0, COLS:]
    lanes = iota((GROUPS, 128), 1)

    def fact(no):
        return jnp.sum(jnp.where(lanes == no, all_facts, 0.0), axis=1, keepdims=True)

    group_no = iota((GROUPS, 1), 0)
    before = group_no < my_group
    same_first = (fact(0) == first_hi) & (fact(1) == first_lo)
    same_last = (fact(2) == first_hi) & (fact(3) == first_lo)
    stop = before & ((fact(4) > 0.0) | jnp.logical_not(same_first))
    last_stop = jnp.max(jnp.where(stop, group_no, -1), axis=0, keepdims=True)
    linked = before & ((group_no > last_stop) | ((group_no == last_stop) & same_last))
    carry_in = jnp.sum(jnp.where(linked, tail_all[:, 0, :COLS], 0.0), axis=0, keepdims=True)

    def sums(blk, carry):
        devs = [peer(me, blk * 8 + sub) for sub in range(8)]
        hot = jnp.concatenate([mask_ref[my_rows(dev)] for dev in devs], axis=0)
        bound = jnp.concatenate([bcol_ref[my_rows(dev)] for dev in devs], axis=0)
        open_run = bound[:, :1] == NEG
        total = jnp.dot(hot, recv[...], preferred_element_type=F32)
        total = (total + jnp.where(open_run, carry_in, 0.0)).astype(BF16)
        for sub, dev in enumerate(devs):
            sums_ref[my_rows(dev)] = total[sub * CAP:(sub + 1) * CAP]
            send = remote(sums_ref.at[my_rows(dev)], ret.at[my_part, my_rows(my_group)], ret_sem, dev)
            if sub == 0:
                @pl.when(blk > 0)
                def _(send=send):
                    send.start()
            else:
                send.start()
        return carry

    lax.fori_loop(0, DEVS // 8, sums, 0)
    ret[my_part, my_rows(my_group)] = sums_ref[my_rows(me)]
    remote(recv.at[pl.ds(0, SLOTS - CAP)], recv.at[pl.ds(0, SLOTS - CAP)], ret_sem, me).wait_recv()

    def unpack(step, carry):
        spot = iota((128, PACK), 1).astype(F32)
        for blk in range(ROWS // 128):
            hot = jnp.where(spot == place_col[blk * 128:(blk + 1) * 128], 1.0, 0.0).astype(BF16)
            for part in range(SPLIT):
                rows = jnp.dot(hot, ret[part], preferred_element_type=F32)
                out_ref[blk * 128:(blk + 1) * 128, part * COLS:(part + 1) * COLS] = rows.astype(BF16)
        return carry

    unpack(0, 0)

    def sent(src):
        remote(src, src, ret_sem, me).wait_send()

    sent(samp_all.at[pl.ds(0, DEVS - 1)])
    sent(meta_all.at[pl.ds(0, DEVS - 1)])
    sent(recv.at[pl.ds(0, SLOTS - CAP)])
    sent(tail_all.at[pl.ds(0, GROUPS - 1)])
    sent(recv.at[pl.ds(0, SLOTS - CAP)])


def solution(mesh):
    def per_device(sort_keys, seg_ids, payload):
        vmem = pl.BlockSpec(memory_space=pltpu.VMEM)
        dma = pltpu.SemaphoreType.DMA
        call = pl.pallas_call(
            kernel,
            out_shape=jax.ShapeDtypeStruct((ROWS, WIDTH), BF16),
            in_specs=[vmem] * 3,
            out_specs=vmem,
            scratch_shapes=[
                pltpu.VMEM((1, DEVS), F32),
                pltpu.VMEM((DEVS, 1, DEVS), F32),
                pltpu.VMEM((SPLIT, PACK, COLS), BF16),
                pltpu.VMEM((SLOTS, COLS), BF16),
                pltpu.VMEM((GROUPS, 1, 128), F32),
                pltpu.VMEM((DEVS, 1, 128), F32),
                pltpu.VMEM((SLOTS, SLOTS), BF16),
                pltpu.VMEM((SLOTS, 128), F32),
                pltpu.VMEM((SLOTS, 128), I32),
                pltpu.VMEM((SLOTS, 128), F32),
                pltpu.VMEM((SLOTS // 128, 1, 128), F32),
                pltpu.VMEM((SLOTS // 128, 1, 128), I32),
                pltpu.VMEM((1, TAILW), F32),
                pltpu.VMEM((GROUPS, 1, TAILW), F32),
                pltpu.VMEM((SLOTS, COLS), BF16),
                pltpu.VMEM((SPLIT, PACK, COLS), BF16),
                dma, dma, dma, dma, dma, dma,
            ],
            compiler_params=pltpu.CompilerParams(collective_id=0, has_side_effects=True, vmem_limit_bytes=62 << 20),
        )
        return call(sort_keys.reshape(1, ROWS), seg_ids.reshape(1, ROWS), payload)

    row_spec = P(('batch', 'group'))
    mat_spec = P(('batch', 'group'), None)
    return jax.shard_map(per_device, mesh=mesh, in_specs=(row_spec, row_spec, mat_spec),
                         out_specs=mat_spec, check_vma=False)
```

```python
import functools

import jax
import jax.numpy as jnp
from jax import lax
from jax.experimental import pallas as pl
from jax.experimental.pallas import tpu as pltpu
from jax.sharding import PartitionSpec as P

F32 = jnp.float32
BF16 = jnp.bfloat16
I32 = jnp.int32
NEG = float('-inf')
POS = float('inf')
MESH = pl.DeviceIdType.MESH

DEVS = 128
ROWS = 512
WIDTH = 2048
LANES = 128
BASE = 16
MORE = 4
FLAG = LANES - 1
HALF = 65536
TALL = 32
RING = 4


class Plan:
    def __init__(self, parts, more):
        self.parts, self.more = parts, more
        self.shift = parts.bit_length() - 1
        self.ranges = DEVS // parts
        self.cols = WIDTH // parts
        self.chunks = self.cols // LANES
        self.full = BASE + more
        self.line = self.cols + (LANES if more else 0)
        self.low = DEVS * BASE
        self.top = DEVS * more
        self.need = self.low + self.top
        self.low_out = self.ranges * BASE
        self.top_out = self.ranges * more
        self.tail = self.cols + LANES


NARROW = Plan(4, MORE)
FULL = Plan(2, 0)


def iota(shape, dim):
    return lax.broadcasted_iota(I32, shape, dim)


def ones_where(hit):
    return jnp.where(hit, 1.0, 0.0)


def hot(hit):
    return ones_where(hit).astype(BF16)


def dot(left, right):
    return jnp.dot(left, right, preferred_element_type=F32)


def along_sublanes(vals):
    return jnp.sum(vals, axis=0, keepdims=True)


def along_lanes(vals):
    return jnp.sum(vals, axis=1, keepdims=True)


def place(me, step):
    core, x, y, z = me & 1, (me >> 1) & (RING - 1), (me >> 3) & (RING - 1), me >> 5
    return (core + step) & 1, ((x + step) & (RING - 1)) << 1, ((y + step) & (RING - 1)) << 3, ((z + step) & (RING - 1)) << 5


def block_of_eight(me, blk):
    found = []
    for turn in range(RING):
        side = place(me, turn)[1] + place(me, turn + (blk & (RING - 1)))[2] + place(me, turn + (blk >> 2))[3]
        found += [side + place(me, flip)[0] for flip in range(2)]
    return found


def kernel(plan, keys_ref, segs_ref, pay_ref, out_ref, flag_ref, samp_msg, samp_all, packed, recv, meta_msg, meta_all,
           mask_ref, kcol_ref, scol_ref, bcol_ref, krow_ref, srow_ref, tail_msg, tail_all, top_ref, sums_ref, ret,
           back_ref, send_sem, samp_sem, meta_sem, row_sem, tail_sem, ret_sem):
    parts, more, cols, chunks = plan.parts, plan.more, plan.cols, plan.chunks
    me = lax.axis_index('group')
    my_range = me >> plan.shift
    my_part = me & (parts - 1)
    barrier = pltpu.get_barrier_semaphore()
    others = [dev for blk in range(DEVS // 8) for dev in block_of_eight(me, blk)][1:]
    rest = pl.ds(0, DEVS - 1)
    most = pl.ds(0, plan.low - BASE)

    def remote(src, dst, recv_sem, dev):
        return pltpu.make_async_remote_copy(src_ref=src, dst_ref=dst, send_sem=send_sem, recv_sem=recv_sem,
                                            device_id={'group': dev}, device_id_type=MESH)

    def arrived(like, sem):
        remote(like, like, sem, others[0]).wait_recv()

    def left(like):
        remote(like, like, ret_sem, others[0]).wait_send()

    def at16(no):
        return pl.ds(pl.multiple_of(no * BASE, BASE), BASE)

    for dev in others:
        pl.semaphore_signal(barrier, inc=1, device_id={'group': dev}, device_id_type=MESH)

    key_row = keys_ref[...]
    seg_row = segs_ref[...]
    square = (ROWS, ROWS)
    eye = iota(square, 0) == iota(square, 1)

    def to_col(row):
        return along_lanes(jnp.where(eye, jnp.broadcast_to(row, square), 0))

    def to_row(col):
        return along_sublanes(jnp.where(eye, jnp.broadcast_to(col, square), 0))

    key_col = to_col(key_row)
    seg_col = to_col(seg_row)
    rank_col = along_lanes(ones_where(key_row < key_col))
    wide = (ROWS, LANES)
    fourth = (iota(wide, 1) * (ROWS // DEVS)).astype(F32)
    samp_msg[...] = along_sublanes(jnp.where(rank_col == fourth, jnp.broadcast_to(key_col, wide), 0.0))
    pl.semaphore_wait(barrier, DEVS - 1)

    for dev in others:
        remote(samp_msg, samp_all.at[me], samp_sem, dev).start()
    samp_all[me] = samp_msg[...]
    arrived(samp_all.at[rest], samp_sem)

    tile = (LANES, LANES)
    counts = []
    for part in range(ROWS // LANES):
        kblk = jnp.broadcast_to(key_col[part * LANES:(part + 1) * LANES], tile)

        def count(step, acc, kblk=kblk):
            for sub in range(8):
                acc = acc + ones_where(samp_all[step * 8 + sub] <= kblk)
            return acc

        counts.append(along_lanes(lax.fori_loop(0, DEVS // 8, count, jnp.zeros(tile, F32))))
    seen_col = jnp.concatenate(counts, axis=0)
    range_col = jnp.maximum(jnp.floor((seen_col - (DEVS // 2 + 1)) * (1.0 / (DEVS * parts))), 0.0)
    range_row = to_row(range_col)
    slot_col = rank_col - along_lanes(ones_where(range_row < range_col))
    low_col = jnp.where(slot_col < BASE, range_col * BASE + slot_col, -1.0)
    low_row = to_row(low_col)
    top_col = jnp.where((slot_col >= BASE) & (slot_col < plan.full), range_col * more + (slot_col - BASE), -1.0)
    spill = ones_where(jnp.max(slot_col, axis=0, keepdims=True) >= plan.full)

    lane = iota(wide, 1)
    lane_val = lane // plan.full
    lane_slot = (lane % plan.full).astype(F32)
    vals = jnp.where(lane_val == 0, key_col, 1.0)
    vals = jnp.where(lane_val == 1, (seg_col // HALF).astype(F32), vals)
    vals = jnp.where(lane_val == 2, (seg_col % HALF).astype(F32), vals)
    vals = jnp.where((lane_slot == slot_col) & (lane_val < 4), vals, 0.0)
    range_b = jnp.broadcast_to(range_col, wide)
    lane_one = iota((1, LANES), 1)
    for dst in range(plan.ranges):
        meta = along_sublanes(jnp.where(range_b == float(dst), vals, 0.0))
        meta_msg[dst] = jnp.where(lane_one == FLAG, spill, meta)
    for dev in others:
        remote(meta_msg.at[dev >> plan.shift], meta_all.at[me], meta_sem, dev).start()
    meta_all[me] = meta_msg[my_range]

    def fold(to, groups):
        return ((to % BASE) // MORE) * groups + (to // BASE) * MORE + to % MORE

    lines = (plan.low_out, plan.low_out)
    hot_low = hot(low_row == iota((plan.low_out, ROWS), 0).astype(F32))
    if more:
        hot_top = hot(to_row(top_col) == iota((plan.top_out, ROWS), 0).astype(F32))
    piles = []
    for part in range(parts):
        pay = pay_ref[:, part * cols:(part + 1) * cols]
        packed[part, :, :cols] = dot(hot_low, pay).astype(BF16)
        if more:
            rows = dot(hot_top, pay).astype(BF16)
            piles.append(jnp.concatenate([rows[:, c * LANES:(c + 1) * LANES] for c in range(chunks)], axis=0))
    if more:
        folded = dot(hot(iota(lines, 1) == fold(iota(lines, 0), plan.top_out)), jnp.concatenate(piles, axis=1)).astype(BF16)
        for part in range(parts):
            packed[part, :, cols:] = folded[:, part * LANES:(part + 1) * LANES]
    for dev in others:
        remote(packed.at[dev & (parts - 1), at16(dev >> plan.shift)], recv.at[at16(me)], row_sem, dev).start()
    recv[at16(me)] = packed[my_part, at16(my_range)]
    arrived(meta_all.at[rest], meta_sem)

    low_tiles = plan.low // LANES
    tiles = plan.need // LANES
    each = LANES // BASE
    quarters = BASE // MORE
    sub = iota(tile, 0)
    lanes = iota(tile, 1)
    diag = sub == lanes

    def read_slots(got, slot):
        found = [along_lanes(jnp.where(lanes == slot + no * plan.full, got, 0.0)) for no in range(4)]
        seg = found[1].astype(I32) * HALF + found[2].astype(I32)
        return found[3] > 0.0, found[0], seg

    def keep(step, live, key, seg):
        rows = pl.ds(step * LANES, LANES)
        kcol_ref[rows] = jnp.broadcast_to(jnp.where(live, key, NEG), tile)
        scol_ref[rows] = jnp.broadcast_to(seg, tile)

    def to_lanes(spot, live, key, seg):
        return along_sublanes(jnp.where(spot, jnp.where(live, key, POS), 0.0)), along_sublanes(jnp.where(spot, seg, 0))

    top_keys, top_segs = [], []
    for step in range(low_tiles):
        got = meta_all[step * each:(step + 1) * each]
        got = jnp.broadcast_to(got, (each, BASE, LANES)).reshape(tile)
        slots = read_slots(got, sub % BASE)
        keep(step, *slots)
        krow_ref[step], srow_ref[step] = to_lanes(diag, *slots)
        if more:
            first = (step % quarters) * (LANES // quarters)
            spot = (sub % BASE < MORE) & (lanes == first + (sub // BASE) * MORE + sub % MORE)
            key, seg = to_lanes(spot, *read_slots(got, BASE + sub % MORE))
            top_keys.append(key)
            top_segs.append(seg)
    for no in range(tiles - low_tiles):
        step = low_tiles + no
        krow_ref[step] = sum(top_keys[no * quarters:(no + 1) * quarters])
        srow_ref[step] = sum(top_segs[no * quarters:(no + 1) * quarters])
        key = along_lanes(jnp.where(diag, jnp.broadcast_to(krow_ref[step], tile), 0.0))
        seg = along_lanes(jnp.where(diag, jnp.broadcast_to(srow_ref[step], tile), 0))
        keep(step, key < POS, key, seg)
    flags = jnp.max(jnp.where(iota((DEVS, LANES), 1) == FLAG, meta_all[:, 0, :], 0.0), axis=0, keepdims=True)
    flag_ref[...] = jnp.broadcast_to(jnp.max(flags, axis=1, keepdims=True), flag_ref.shape)

    def masks(step, carry):
        rows = pl.ds(pl.multiple_of(step * TALL, TALL), TALL)
        kcol = kcol_ref[rows]
        scol = scol_ref[rows]
        best = jnp.full((TALL, LANES), NEG, F32)
        for t in range(tiles):
            best = jnp.maximum(best, jnp.where((krow_ref[t] < kcol) & (srow_ref[t] != scol), krow_ref[t], NEG))
        bound = jnp.broadcast_to(jnp.max(best, axis=1, keepdims=True), best.shape)
        bcol_ref[rows] = bound
        for t in range(tiles):
            mask_ref[rows, t * LANES:(t + 1) * LANES] = hot((krow_ref[t] > bound) & (krow_ref[t] <= kcol))
        return carry

    lax.fori_loop(0, plan.need // TALL, masks, 0)

    krow = [krow_ref[t] for t in range(tiles)]
    srow = [srow_ref[t] for t in range(tiles)]

    def over(items, join, red):
        return red(functools.reduce(join, items), axis=1, keepdims=True)

    key_last = over([jnp.where(k < POS, k, NEG) for k in krow], jnp.maximum, jnp.max)
    key_first = over(krow, jnp.minimum, jnp.min)

    def pick(key):
        seg = over([jnp.where(k == key, s, 0) for k, s in zip(krow, srow)], jnp.add, jnp.sum)
        return seg, [(seg // HALF).astype(F32), (seg % HALF).astype(F32)]

    seg_last, last = pick(key_last)
    _, first = pick(key_first)
    cut = over([jnp.where((k < POS) & (s != seg_last), k, NEG) for k, s in zip(krow, srow)], jnp.maximum, jnp.max)
    tail_hot = jnp.concatenate([ones_where((k > cut) & (k < POS)) for k in krow], axis=1)
    tail_hot = jnp.broadcast_to(tail_hot, (BASE, plan.need)).astype(BF16)
    facts = jnp.zeros((1, LANES), F32)
    for no, val in enumerate(first + last + [ones_where(cut > NEG)]):
        facts = jnp.where(lane_one == no, val, facts)
    arrived(recv.at[most], row_sem)

    pile = LANES * 2
    piled = pile // quarters
    to, at = iota((pile, pile), 0), iota((pile, pile), 1)
    if more:
        widen = hot(to == fold(at, piled))
        for blk in range(plan.low // pile):
            full = dot(widen, recv[blk * pile:(blk + 1) * pile, cols:]).astype(BF16)
            for c in range(chunks):
                top_ref[blk * piled:(blk + 1) * piled, c * LANES:(c + 1) * LANES] = full[c * piled:(c + 1) * piled]

    def apply(mask):
        total = dot(mask[:, :plan.low], recv[:, :cols])
        return total + dot(mask[:, plan.low:], top_ref[...]) if more else total

    tail_msg[:, :cols] = apply(tail_hot)[:1]
    tail_msg[:, cols:] = facts
    for step in range(1, plan.ranges):
        remote(tail_msg, tail_all.at[my_range], tail_sem, (me + step * parts) & (DEVS - 1)).start()
    tail_all[my_range] = tail_msg[...]
    tails = tail_all.at[pl.ds(0, plan.ranges - 1)]
    arrived(tails, tail_sem)

    all_facts = tail_all[:, 0, cols:]
    fact_lane = iota((plan.ranges, LANES), 1)
    fact = [along_lanes(jnp.where(fact_lane == no, all_facts, 0.0)) for no in range(5)]
    range_no = iota((plan.ranges, 1), 0)
    before = range_no < my_range
    same_first = (fact[0] == first[0]) & (fact[1] == first[1])
    same_last = (fact[2] == first[0]) & (fact[3] == first[1])
    stop = before & ((fact[4] > 0.0) | jnp.logical_not(same_first))
    last_stop = jnp.max(jnp.where(stop, range_no, -1), axis=0, keepdims=True)
    linked = before & ((range_no > last_stop) | ((range_no == last_stop) & same_last))
    carry_in = along_sublanes(jnp.where(linked, tail_all[:, 0, :cols], 0.0))

    def finish(mask, bound):
        return (apply(mask) + jnp.where(bound[:, :1] == NEG, carry_in, 0.0)).astype(BF16)

    if more:
        narrow = hot(at == fold(to, piled))

        def top_sums(blk, carry):
            rows = pl.ds(pl.multiple_of(plan.low + blk * LANES, LANES), LANES)
            total = finish(mask_ref[rows], bcol_ref[rows])
            for no in range(LANES // piled):
                rows = total[no * piled:(no + 1) * piled]
                rows = jnp.concatenate([rows[:, c * LANES:(c + 1) * LANES] for c in range(chunks)], axis=0)
                start = pl.multiple_of((blk * (LANES // piled) + no) * pile, pile)
                sums_ref[pl.ds(start, pile), cols:] = dot(narrow, rows).astype(BF16)
            return carry

        lax.fori_loop(0, plan.top // LANES, top_sums, 0)

    def sums(blk, carry):
        devs = block_of_eight(me, blk)
        total = finish(jnp.concatenate([mask_ref[at16(dev)] for dev in devs], axis=0),
                       jnp.concatenate([bcol_ref[at16(dev)] for dev in devs], axis=0))
        for no, dev in enumerate(devs):
            sums_ref[at16(dev), :cols] = total[no * BASE:(no + 1) * BASE]
            send = remote(sums_ref.at[at16(dev)], ret.at[my_part, at16(my_range)], ret_sem, dev)
            pl.when(blk + no > 0)(send.start)
        return carry

    lax.fori_loop(0, DEVS // 8, sums, 0)
    ret[my_part, at16(my_range)] = sums_ref[at16(me)]
    arrived(recv.at[most], ret_sem)

    if more:
        piles = jnp.concatenate([ret[part, :, cols:] for part in range(parts)], axis=1)
        piles = dot(hot(iota(lines, 0) == fold(iota(lines, 1), plan.top_out)), piles).astype(BF16)
        for part in range(parts):
            for c in range(chunks):
                start = part * cols + c * LANES
                back_ref[:, start:start + LANES] = (
                    piles[c * plan.top_out:(c + 1) * plan.top_out, part * LANES:(part + 1) * LANES])
        hot_top = hot(top_col == iota((ROWS, plan.top_out), 1).astype(F32))
    hot_low = hot(low_col == iota((ROWS, plan.low_out), 1).astype(F32))
    for part in range(parts):
        here = slice(part * cols, (part + 1) * cols)
        rows = dot(hot_low, ret[part, :, :cols])
        if more:
            rows = rows + dot(hot_top, back_ref[:, here])
        out_ref[:, here] = rows.astype(BF16)

    for like in (samp_all.at[rest], meta_all.at[rest], recv.at[most], tails, recv.at[most]):
        left(like)


def run(plan, call_id, keys, segs, payload):
    vmem = pl.BlockSpec(memory_space=pltpu.VMEM)
    shapes = [
        ((1, LANES), F32),
        ((DEVS, 1, LANES), F32),
        ((plan.parts, plan.low_out, plan.line), BF16),
        ((plan.low, plan.line), BF16),
        ((plan.ranges, 1, LANES), F32),
        ((DEVS, 1, LANES), F32),
        ((plan.need, plan.need), BF16),
        ((plan.need, LANES), F32),
        ((plan.need, LANES), I32),
        ((plan.need, LANES), F32),
        ((plan.need // LANES, 1, LANES), F32),
        ((plan.need // LANES, 1, LANES), I32),
        ((1, plan.tail), F32),
        ((plan.ranges, 1, plan.tail), F32),
        ((max(plan.top, BASE), plan.cols), BF16),
        ((plan.low, plan.line), BF16),
        ((plan.parts, plan.low_out, plan.line), BF16),
        ((max(plan.top_out, BASE), WIDTH), BF16),
    ]
    return pl.pallas_call(
        functools.partial(kernel, plan),
        out_shape=(jax.ShapeDtypeStruct((ROWS, WIDTH), BF16), jax.ShapeDtypeStruct((8, LANES), F32)),
        in_specs=[vmem] * 3,
        out_specs=(vmem, vmem),
        scratch_shapes=[pltpu.VMEM(*shape) for shape in shapes] + [pltpu.SemaphoreType.DMA] * 6,
        compiler_params=pltpu.CompilerParams(collective_id=call_id, has_side_effects=True, vmem_limit_bytes=62 << 20),
    )(keys, segs, payload)


def solution(mesh):
    def per_device(sort_keys, seg_ids, payload):
        args = (sort_keys.reshape(1, ROWS), seg_ids.reshape(1, ROWS), payload)
        out, flag = run(NARROW, 0, *args)
        return lax.cond(flag[0, 0] > 0.0, lambda done: run(FULL, 1, *args)[0], lambda done: done, out)

    row_spec = P(('batch', 'group'))
    mat_spec = P(('batch', 'group'), None)
    return jax.shard_map(per_device, mesh=mesh, in_specs=(row_spec, row_spec, mat_spec),
                         out_specs=mat_spec, check_vma=False)
```

```python
import functools

import jax
import jax.numpy as jnp
from jax import lax
from jax.experimental import pallas as pl
from jax.experimental.pallas import tpu as pltpu
from jax.sharding import PartitionSpec as P

F32 = jnp.float32
BF16 = jnp.bfloat16
I32 = jnp.int32
NEG = float('-inf')
POS = float('inf')
MESH = pl.DeviceIdType.MESH

DEVS = 128
ROWS = 512
WIDTH = 2048
LANES = 128
BASE = 16
MORE = 4
FLAG = LANES - 1
TALL = 32
EARLY = 32
RING = 4


class Plan:
    def __init__(self, parts, more, stride):
        self.parts, self.more, self.stride = parts, more, stride
        self.shift = parts.bit_length() - 1
        self.ranges = DEVS // parts
        self.per = ROWS // stride
        self.share = LANES // self.per
        self.cols = WIDTH // parts
        self.half = self.cols // 2
        self.chunks = self.cols // LANES
        self.full = BASE + more
        self.extra = LANES if more else 0
        self.long = self.half + self.extra
        self.low = DEVS * BASE
        self.top = DEVS * more
        self.need = self.low + self.top
        self.low_out = self.ranges * BASE
        self.top_out = self.ranges * more


NARROW = Plan(4, MORE, BASE)
FULL = Plan(2, 0, 4)


def iota(shape, dim):
    return lax.broadcasted_iota(I32, shape, dim)


def ones_where(hit):
    return jnp.where(hit, 1.0, 0.0)


def hot(hit):
    return ones_where(hit).astype(BF16)


def dot(left, right):
    return jnp.dot(left, right, preferred_element_type=F32)


def along_sublanes(vals):
    return jnp.sum(vals, axis=0, keepdims=True)


def along_lanes(vals):
    return jnp.sum(vals, axis=1, keepdims=True)


def fold(to, groups):
    return ((to & (BASE - 1)) >> 2) * groups + (to >> 4) * MORE + (to & (MORE - 1))


def fold_hot(size, groups):
    return hot(fold(iota((size, 1), 0), groups) == iota((1, size), 1))


def unfold_hot(size, groups):
    return hot(iota((size, 1), 0) == fold(iota((1, size), 1), groups))


def stack(rows, chunks):
    return jnp.concatenate([rows[:, c * LANES:(c + 1) * LANES] for c in range(chunks)], axis=0)


def place(me, step):
    core, x, y, z = me & 1, (me >> 1) & (RING - 1), (me >> 3) & (RING - 1), me >> 5
    return (core + step) & 1, ((x + step) & (RING - 1)) << 1, ((y + step) & (RING - 1)) << 3, ((z + step) & (RING - 1)) << 5


def other_devices(me):
    places = [place(me, step) for step in range(RING)]
    found = []
    for blk in range(DEVS // 8):
        for turn in range(RING):
            side = places[turn][1] + places[(turn + blk) % RING][2] + places[(turn + blk // RING) % RING][3]
            found += [side + places[flip][0] for flip in range(2)]
    return found[1:]


def kernel(plan, keys_ref, segs_ref, pay_hbm, out_ref, flag_ref, pay_ref, samp_msg, samp_all, fold_ref, packed0, packed1,
           recv0, recv1, meta_msg, meta_all, mask_ref, kcol_ref, scol_ref, bcol_ref, krow_ref, srow_ref, tail_msg0,
           tail_msg1, tail_all0, tail_all1, top_ref, acc_ref, top_done, sums0, sums1, ret0, ret1, back_ref, hot_low_ref,
           hot_top_ref, pay_sem, send_sem, samp_sem, meta_sem, row_sem0, row_sem1, tail_sem0, tail_sem1, ret_sem0,
           ret_sem1):
    parts, more, cols, half, chunks = plan.parts, plan.more, plan.cols, plan.half, plan.chunks
    me = lax.axis_index('group')
    my_range = me >> plan.shift
    my_part = me & (parts - 1)
    barrier = pltpu.get_barrier_semaphore()
    others = other_devices(me)
    rest = pl.ds(0, DEVS - 1)
    most = pl.ds(0, plan.low - BASE)

    def remote(src, dst, recv_sem, dev):
        return pltpu.make_async_remote_copy(src_ref=src, dst_ref=dst, send_sem=send_sem, recv_sem=recv_sem,
                                            device_id={'group': dev}, device_id_type=MESH)

    def arrived(like, sem):
        remote(like, like, sem, others[0]).wait_recv()

    def left(like):
        remote(like, like, ret_sem0, others[0]).wait_send()

    def at16(no):
        return pl.ds(pl.multiple_of(no * BASE, BASE), BASE)

    for dev in others:
        pl.semaphore_signal(barrier, inc=1, device_id={'group': dev}, device_id_type=MESH)
    fetch = pltpu.make_async_copy(pay_hbm, pay_ref, pay_sem)
    fetch.start()

    key_row = keys_ref[...]
    seg_row = segs_ref[...]
    square = (ROWS, ROWS)
    eye = iota(square, 0) == iota(square, 1)

    def to_col(row):
        return along_lanes(jnp.where(eye, jnp.broadcast_to(row, square), 0))

    def to_row(col):
        return along_sublanes(jnp.where(eye, jnp.broadcast_to(col, square), 0))

    key_col = to_col(key_row)
    rank_col = along_lanes(ones_where(key_row < key_col))
    wide = (ROWS, LANES)
    lane_one = iota((1, LANES), 1)
    chosen = ((lane_one - (me & (plan.share - 1)) * plan.per) * plan.stride).astype(F32)
    samp_msg[...] = along_sublanes(jnp.where(rank_col == chosen, jnp.broadcast_to(key_col, wide), 0.0))
    pl.semaphore_wait(barrier, DEVS - 1)

    for dev in others:
        remote(samp_msg, samp_all.at[me], samp_sem, dev).start()
    samp_all[me] = samp_msg[...]
    if more:
        fold_ref[...] = fold_hot(plan.low_out, plan.top_out)
    seg_col = to_col(seg_row)
    arrived(samp_all.at[rest], samp_sem)

    tile = (LANES, LANES)
    counts = []
    for part in range(ROWS // LANES):
        kblk = jnp.broadcast_to(key_col[part * LANES:(part + 1) * LANES], tile)

        def count(step, acc, kblk=kblk):
            for sub in range(8):
                row = (step * 8 + sub) * plan.share
                acc = acc + ones_where(sum(samp_all[row + no] for no in range(plan.share)) <= kblk)
            return acc

        counts.append(along_lanes(lax.fori_loop(0, plan.per // 8, count, jnp.zeros(tile, F32))))
    seen_col = jnp.concatenate(counts, axis=0)
    per_range = DEVS * plan.per // plan.ranges
    range_col = jnp.maximum(jnp.floor((seen_col - (DEVS // 2 + 1)) * (1.0 / per_range)), 0.0)
    range_row = to_row(range_col)
    slot_col = rank_col - along_lanes(ones_where(range_row < range_col))
    low_col = jnp.where(slot_col < BASE, range_col * BASE + slot_col, -1.0)
    low_row = to_row(low_col)
    top_col = jnp.where((slot_col >= BASE) & (slot_col < plan.full), range_col * more + (slot_col - BASE), -1.0)
    spill = ones_where(jnp.max(slot_col, axis=0, keepdims=True) >= plan.full)

    hot_low = hot(low_row == iota((plan.low_out, 1), 0).astype(F32))
    if more:
        hot_top = hot(to_row(top_col) == iota((plan.top_out, 1), 0).astype(F32))
    fetch.wait()
    piles = []
    for part in range(parts):
        start = part * cols
        packed0[part, :, :half] = dot(hot_low, pay_ref[:, start:start + half]).astype(BF16)
        if more:
            piles.append(stack(dot(hot_top, pay_ref[:, start:start + cols]).astype(BF16), chunks))
    if more:
        folded = dot(fold_ref[...], jnp.concatenate(piles, axis=1)).astype(BF16)
        for part in range(parts):
            packed0[part, :, half:] = folded[:, part * LANES:(part + 1) * LANES]

    def send_rows(devs, src, dst, sem):
        for dev in devs:
            remote(src.at[dev & (parts - 1), at16(dev >> plan.shift)], dst.at[at16(me)], sem, dev).start()

    send_rows(others[:EARLY], packed0, recv0, row_sem0)

    lane_val = lane_one // plan.full
    lane_slot = (lane_one % plan.full).astype(F32)
    vals = jnp.where(lane_val == 0, key_col, 1.0)
    vals = jnp.where(lane_val == 1, (seg_col >> 16).astype(F32), vals)
    vals = jnp.where(lane_val == 2, (seg_col & 65535).astype(F32), vals)
    vals = jnp.where((lane_slot == slot_col) & (lane_val < 4), vals, 0.0)
    range_b = jnp.broadcast_to(range_col, wide)
    for dst in range(plan.ranges):
        meta = along_sublanes(jnp.where(range_b == float(dst), vals, 0.0))
        meta_msg[dst] = jnp.where(lane_one == FLAG, spill, meta)
    for dev in others:
        remote(meta_msg.at[dev >> plan.shift], meta_all.at[me], meta_sem, dev).start()
    meta_all[me] = meta_msg[my_range]
    send_rows(others[EARLY:], packed0, recv0, row_sem0)

    for part in range(parts):
        start = part * cols + half
        packed1[part] = dot(hot_low, pay_ref[:, start:start + half]).astype(BF16)
    send_rows(others, packed1, recv1, row_sem1)
    recv0[at16(me)] = packed0[my_part, at16(my_range)]
    recv1[at16(me)] = packed1[my_part, at16(my_range)]
    arrived(meta_all.at[rest], meta_sem)

    low_tiles = plan.low // LANES
    tiles = plan.need // LANES
    each = LANES // BASE
    quarters = BASE // MORE
    sub = iota((LANES, 1), 0)
    diag = sub == lane_one

    def read_slots(got, slot):
        found = [along_lanes(jnp.where(lane_one == slot + no * plan.full, got, 0.0)) for no in range(4)]
        seg = (found[1].astype(I32) << 16) + found[2].astype(I32)
        return found[3] > 0.0, found[0], seg

    def keep(step, live, key, seg):
        rows = pl.ds(step * LANES, LANES)
        kcol_ref[rows] = jnp.broadcast_to(jnp.where(live, key, NEG), tile)
        scol_ref[rows] = jnp.broadcast_to(seg, tile)

    def to_lanes(spot, live, key, seg):
        return along_sublanes(jnp.where(spot, jnp.where(live, key, POS), 0.0)), along_sublanes(jnp.where(spot, seg, 0))

    top_keys, top_segs = [], []
    for step in range(low_tiles):
        got = meta_all[step * each:(step + 1) * each]
        got = jnp.broadcast_to(got, (each, BASE, LANES)).reshape(tile)
        slots = read_slots(got, sub & (BASE - 1))
        keep(step, *slots)
        krow_ref[step], srow_ref[step] = to_lanes(diag, *slots)
        if more:
            first = (step % quarters) * (LANES // quarters)
            spot = (lane_one == first + (sub >> 4) * MORE + (sub & (MORE - 1))) & ((sub & (BASE - 1)) < MORE)
            key, seg = to_lanes(spot, *read_slots(got, BASE + (sub & (MORE - 1))))
            top_keys.append(key)
            top_segs.append(seg)
    for no in range(tiles - low_tiles):
        step = low_tiles + no
        krow_ref[step] = sum(top_keys[no * quarters:(no + 1) * quarters])
        srow_ref[step] = sum(top_segs[no * quarters:(no + 1) * quarters])
        key = along_lanes(jnp.where(diag, jnp.broadcast_to(krow_ref[step], tile), 0.0))
        seg = along_lanes(jnp.where(diag, jnp.broadcast_to(srow_ref[step], tile), 0))
        keep(step, key < POS, key, seg)
    flags = jnp.max(jnp.where(lane_one == FLAG, meta_all[:, 0, :], 0.0), axis=0, keepdims=True)
    flag_ref[...] = jnp.broadcast_to(jnp.max(flags, axis=1, keepdims=True), flag_ref.shape)

    def masks(step, carry):
        rows = pl.ds(pl.multiple_of(step * TALL, TALL), TALL)
        kcol = kcol_ref[rows]
        scol = scol_ref[rows]
        best = jnp.full((TALL, LANES), NEG, F32)
        for t in range(tiles):
            best = jnp.maximum(best, jnp.where((krow_ref[t] < kcol) & (srow_ref[t] != scol), krow_ref[t], NEG))
        bound = jnp.broadcast_to(jnp.max(best, axis=1, keepdims=True), best.shape)
        bcol_ref[rows] = bound
        for t in range(tiles):
            mask_ref[rows, t * LANES:(t + 1) * LANES] = hot((krow_ref[t] > bound) & (krow_ref[t] <= kcol))
        return carry

    lax.fori_loop(0, plan.need // TALL, masks, 0)

    krow = [krow_ref[t] for t in range(tiles)]
    srow = [srow_ref[t] for t in range(tiles)]

    def over(items, join, red):
        return red(functools.reduce(join, items), axis=1, keepdims=True)

    key_last = over([jnp.where(k < POS, k, NEG) for k in krow], jnp.maximum, jnp.max)
    key_first = over(krow, jnp.minimum, jnp.min)

    def pick(key):
        seg = over([jnp.where(k == key, s, 0) for k, s in zip(krow, srow)], jnp.add, jnp.sum)
        return seg, [(seg >> 16).astype(F32), (seg & 65535).astype(F32)]

    seg_last, last = pick(key_last)
    _, first = pick(key_first)
    cut = over([jnp.where((k < POS) & (s != seg_last), k, NEG) for k, s in zip(krow, srow)], jnp.maximum, jnp.max)
    tail_hot = jnp.concatenate([ones_where((k > cut) & (k < POS)) for k in krow], axis=1)
    tail_hot = jnp.broadcast_to(tail_hot, (BASE, plan.need)).astype(BF16)
    facts = jnp.zeros((1, LANES), F32)
    for no, val in enumerate(first + last + [ones_where(cut > NEG)]):
        facts = jnp.where(lane_one == no, val, facts)

    hot_low_ref[...] = hot(low_col == iota((1, plan.low_out), 1).astype(F32))
    if more:
        fold_ref[...] = unfold_hot(plan.low_out, plan.top_out)
        hot_top_ref[...] = hot(top_col == iota((1, plan.top_out), 1).astype(F32))

    def apply(mask, recv, no):
        total = dot(mask[:, :plan.low], recv[:, :half])
        return total + dot(mask[:, plan.low:], top_ref[:, no * half:(no + 1) * half]) if more else total

    def send_tail(msg, dst, sem):
        for step in range(1, plan.ranges):
            remote(msg, dst.at[my_range], sem, (me + step * parts) & (DEVS - 1)).start()
        dst[my_range] = msg[...]

    big = 256

    def products(recv, no):
        def step(blk, carry):
            rows = pl.ds(pl.multiple_of(blk * big, big), big)
            acc_ref[rows] = apply(mask_ref[rows], recv, no)
            return carry

        lax.fori_loop(0, plan.need // big, step, 0)

    arrived(recv0.at[most], row_sem0)
    piled = big // quarters
    if more:
        widen = unfold_hot(big, piled)
        for blk in range(plan.low // big):
            full = dot(widen, recv0[blk * big:(blk + 1) * big, half:]).astype(BF16)
            for c in range(chunks):
                top_ref[blk * piled:(blk + 1) * piled, c * LANES:(c + 1) * LANES] = full[c * piled:(c + 1) * piled]
    tail_msg0[:, :half] = apply(tail_hot, recv0, 0)[:1]
    tail_msg0[:, half:] = facts
    send_tail(tail_msg0, tail_all0, tail_sem0)
    products(recv0, 0)
    arrived(recv1.at[most], row_sem1)
    tail_msg1[...] = apply(tail_hot, recv1, 1)[:1]
    send_tail(tail_msg1, tail_all1, tail_sem1)
    tails0 = tail_all0.at[pl.ds(0, plan.ranges - 1)]
    tails1 = tail_all1.at[pl.ds(0, plan.ranges - 1)]
    arrived(tails0, tail_sem0)

    fact = [along_lanes(jnp.where(lane_one == no, tail_all0[:, 0, half:], 0.0)) for no in range(5)]
    range_no = iota((plan.ranges, 1), 0)
    before = range_no < my_range
    same_first = (fact[0] == first[0]) & (fact[1] == first[1])
    same_last = (fact[2] == first[0]) & (fact[3] == first[1])
    stop = before & ((fact[4] > 0.0) | jnp.logical_not(same_first))
    last_stop = jnp.max(jnp.where(stop, range_no, -1), axis=0, keepdims=True)
    linked = before & ((range_no > last_stop) | ((range_no == last_stop) & same_last))

    def finish(tails, no, sums):
        carry_in = along_sublanes(jnp.where(linked, tails[:, 0, :half], 0.0))

        def closed(rows):
            return (acc_ref[rows] + jnp.where(bcol_ref[rows][:, :1] == NEG, carry_in, 0.0)).astype(BF16)

        def step(blk, carry):
            rows = pl.ds(pl.multiple_of(blk * big, big), big)
            sums[rows, :half] = closed(rows)
            return carry

        lax.fori_loop(0, plan.low // big, step, 0)
        if more:
            top_done[:, no * half:(no + 1) * half] = closed(pl.ds(plan.low, plan.top))

    def send_back(src, dst, sem):
        for dev in others:
            remote(src.at[at16(dev)], dst.at[my_part, at16(my_range)], sem, dev).start()
        dst[my_part, at16(my_range)] = src[at16(me)]

    finish(tail_all0, 0, sums0)
    send_back(sums0, ret0, ret_sem0)

    products(recv1, 1)
    arrived(tails1, tail_sem1)
    finish(tail_all1, 1, sums1)
    if more:
        narrow = fold_hot(big, piled)
        for blk in range(plan.top // piled):
            pile = stack(top_done[blk * piled:(blk + 1) * piled], chunks)
            sums1[blk * big:(blk + 1) * big, half:] = dot(narrow, pile).astype(BF16)
    send_back(sums1, ret1, ret_sem1)

    arrived(recv1.at[most], ret_sem0)
    if not more:
        for part in range(parts):
            start = part * cols
            out_ref[:, start:start + half] = dot(hot_low_ref[...], ret0[part]).astype(BF16)
    else:
        for part in range(parts):
            back_ref[:, part * half:(part + 1) * half] = dot(hot_low_ref[...], ret0[part])
    arrived(recv0.at[most], ret_sem1)
    if more:
        piles = jnp.concatenate([ret1[part, :, half:] for part in range(parts)], axis=1)
        piles = dot(fold_ref[...], piles).astype(BF16)
    for part in range(parts):
        start = part * cols
        rows = dot(hot_low_ref[...], ret1[part, :, :half])
        if more:
            top_rows = jnp.concatenate([piles[c * plan.top_out:(c + 1) * plan.top_out, part * LANES:(part + 1) * LANES]
                                        for c in range(chunks)], axis=1)
            top_rows = dot(hot_top_ref[...], top_rows)
            rows = rows + top_rows[:, half:]
            out_ref[:, start:start + half] = (back_ref[:, part * half:(part + 1) * half] + top_rows[:, :half]).astype(BF16)
        out_ref[:, start + half:start + cols] = rows.astype(BF16)

    for like in (samp_all.at[rest], meta_all.at[rest], recv0.at[most], recv1.at[most], tails0, tails1, recv0.at[most],
                 recv1.at[most]):
        left(like)


def run(plan, call_id, keys, segs, payload):
    vmem = pl.BlockSpec(memory_space=pltpu.VMEM)
    shapes = [
        ((ROWS, WIDTH), BF16),
        ((1, LANES), F32),
        ((DEVS, 1, LANES), F32),
        ((plan.low_out, plan.low_out) if plan.more else (BASE, LANES), BF16),
        ((plan.parts, plan.low_out, plan.long), BF16),
        ((plan.parts, plan.low_out, plan.half), BF16),
        ((plan.low, plan.long), BF16),
        ((plan.low, plan.half), BF16),
        ((plan.ranges, 1, LANES), F32),
        ((DEVS, 1, LANES), F32),
        ((plan.need, plan.need), BF16),
        ((plan.need, LANES), F32),
        ((plan.need, LANES), I32),
        ((plan.need, LANES), F32),
        ((plan.need // LANES, 1, LANES), F32),
        ((plan.need // LANES, 1, LANES), I32),
        ((1, plan.half + LANES), F32),
        ((1, plan.half), F32),
        ((plan.ranges, 1, plan.half + LANES), F32),
        ((plan.ranges, 1, plan.half), F32),
        ((max(plan.top, BASE), plan.cols), BF16),
        ((plan.need, plan.half), F32),
        ((max(plan.top, BASE), plan.cols), BF16),
        ((plan.low, plan.half), BF16),
        ((plan.low, plan.long), BF16),
        ((plan.parts, plan.low_out, plan.half), BF16),
        ((plan.parts, plan.low_out, plan.long), BF16),
        ((ROWS, WIDTH // 2) if plan.more else (8, LANES), F32),
        ((ROWS, plan.low_out), BF16),
        ((ROWS, max(plan.top_out, LANES)), BF16),
    ]
    return pl.pallas_call(
        functools.partial(kernel, plan),
        out_shape=(jax.ShapeDtypeStruct((ROWS, WIDTH), BF16), jax.ShapeDtypeStruct((8, LANES), F32)),
        in_specs=[vmem, vmem, pl.BlockSpec(memory_space=pl.ANY)],
        out_specs=(vmem, vmem),
        scratch_shapes=[pltpu.VMEM(*shape) for shape in shapes] + [pltpu.SemaphoreType.DMA] * 10,
        compiler_params=pltpu.CompilerParams(collective_id=call_id, has_side_effects=True, vmem_limit_bytes=62 << 20),
    )(keys, segs, payload)


def solution(mesh):
    def per_device(sort_keys, seg_ids, payload):
        args = (sort_keys.reshape(1, ROWS), seg_ids.reshape(1, ROWS), payload)
        out, flag = run(NARROW, 0, *args)
        return lax.cond(flag[0, 0] > 0.0, lambda done: run(FULL, 1, *args)[0], lambda done: done, out)

    row_spec = P(('batch', 'group'))
    mat_spec = P(('batch', 'group'), None)
    return jax.shard_map(per_device, mesh=mesh, in_specs=(row_spec, row_spec, mat_spec),
                         out_specs=mat_spec, check_vma=False)
```

```python
import functools

import jax
import jax.numpy as jnp
from jax import lax
from jax.experimental import pallas as pl
from jax.experimental.pallas import tpu as pltpu
from jax.sharding import PartitionSpec as P

F32 = jnp.float32
BF16 = jnp.bfloat16
I32 = jnp.int32
NEG = float('-inf')
POS = float('inf')
MESH = pl.DeviceIdType.MESH

DEVS = 128
ROWS = 512
WIDTH = 2048
LANES = 128
BASE = 16
MORE = 4
FLAG = LANES - 1
TALL = 32
EARLY = 32
RING = 4


class Plan:
    def __init__(self, parts, more, stride):
        self.parts, self.more, self.stride = parts, more, stride
        self.shift = parts.bit_length() - 1
        self.ranges = DEVS // parts
        self.per = ROWS // stride
        self.share = LANES // self.per
        self.cols = WIDTH // parts
        self.half = self.cols // 2
        self.chunks = self.cols // LANES
        self.full = BASE + more
        self.extra = LANES if more else 0
        self.long = self.half + self.extra
        self.low = DEVS * BASE
        self.top = DEVS * more
        self.need = self.low + self.top
        self.low_out = self.ranges * BASE
        self.top_out = self.ranges * more


NARROW = Plan(4, MORE, BASE)
FULL = Plan(2, 0, 4)


def iota(shape, dim):
    return lax.broadcasted_iota(I32, shape, dim)


def ones_where(hit):
    return jnp.where(hit, 1.0, 0.0)


def hot(hit):
    return ones_where(hit).astype(BF16)


def dot(left, right):
    return jnp.dot(left, right, preferred_element_type=F32)


def along_sublanes(vals):
    return jnp.sum(vals, axis=0, keepdims=True)


def along_lanes(vals):
    return jnp.sum(vals, axis=1, keepdims=True)


def fold(to, groups):
    return ((to & (BASE - 1)) >> 2) * groups + (to >> 4) * MORE + (to & (MORE - 1))


def fold_hot(size, groups):
    return hot(fold(iota((size, 1), 0), groups) == iota((1, size), 1))


def unfold_hot(size, groups):
    return hot(iota((size, 1), 0) == fold(iota((1, size), 1), groups))


def stack(rows, chunks):
    return jnp.concatenate([rows[:, c * LANES:(c + 1) * LANES] for c in range(chunks)], axis=0)


def place(me, step):
    core, x, y, z = me & 1, (me >> 1) & (RING - 1), (me >> 3) & (RING - 1), me >> 5
    return (core + step) & 1, ((x + step) & (RING - 1)) << 1, ((y + step) & (RING - 1)) << 3, ((z + step) & (RING - 1)) << 5


def other_devices(me):
    places = [place(me, step) for step in range(RING)]
    found = []

    def add(along_x, along_y, along_z, flip):
        found.append(places[along_z % RING][3] + places[along_y % RING][2] + places[along_x][1] + places[flip][0])

    for near in (True, False):
        for flip in range(2):
            for along_z in range(RING):
                for along_y in range(RING):
                    if near:
                        add(1, along_y, along_z, flip)
                        add(3, along_y + 2, along_z + 2, flip)
                    else:
                        add(2, along_y + 2, along_z + 2, flip)
                        if along_y or along_z or flip:
                            add(0, along_y, along_z, flip)
    return found


def kernel(plan, keys_ref, segs_ref, pay_hbm, out_ref, flag_ref, pay_ref, samp_msg, samp_all, fold_ref, packed0, packed1,
           recv0, recv1, meta_msg, meta_all, mask_ref, kcol_ref, scol_ref, bcol_ref, krow_ref, srow_ref, tail_msg0,
           tail_msg1, tail_all0, tail_all1, top_ref, acc_ref, top_done, sums0, sums1, ret0, ret1, back_ref, hot_low_ref,
           hot_top_ref, pay_sem, send_sem, samp_sem, meta_sem, row_sem0, row_sem1, tail_sem0, tail_sem1, ret_sem0,
           ret_sem1):
    parts, more, cols, half, chunks = plan.parts, plan.more, plan.cols, plan.half, plan.chunks
    me = lax.axis_index('group')
    my_range = me >> plan.shift
    my_part = me & (parts - 1)
    barrier = pltpu.get_barrier_semaphore()
    others = other_devices(me)
    rest = pl.ds(0, DEVS - 1)
    most = pl.ds(0, plan.low - BASE)

    def remote(src, dst, recv_sem, dev):
        return pltpu.make_async_remote_copy(src_ref=src, dst_ref=dst, send_sem=send_sem, recv_sem=recv_sem,
                                            device_id={'group': dev}, device_id_type=MESH)

    def arrived(like, sem):
        remote(like, like, sem, others[0]).wait_recv()

    def left(like):
        remote(like, like, ret_sem0, others[0]).wait_send()

    def at16(no):
        return pl.ds(pl.multiple_of(no * BASE, BASE), BASE)

    for dev in others:
        pl.semaphore_signal(barrier, inc=1, device_id={'group': dev}, device_id_type=MESH)
    fetch = pltpu.make_async_copy(pay_hbm, pay_ref, pay_sem)
    fetch.start()

    key_row = keys_ref[...]
    seg_row = segs_ref[...]
    square = (ROWS, ROWS)
    eye = iota(square, 0) == iota(square, 1)

    def to_col(row):
        return along_lanes(jnp.where(eye, jnp.broadcast_to(row, square), 0))

    def to_row(col):
        return along_sublanes(jnp.where(eye, jnp.broadcast_to(col, square), 0))

    key_col = to_col(key_row)
    rank_col = along_lanes(ones_where(key_row < key_col))
    wide = (ROWS, LANES)
    lane_one = iota((1, LANES), 1)
    chosen = ((lane_one - (me & (plan.share - 1)) * plan.per) * plan.stride).astype(F32)
    samp_msg[...] = along_sublanes(jnp.where(rank_col == chosen, jnp.broadcast_to(key_col, wide), 0.0))
    pl.semaphore_wait(barrier, DEVS - 1)

    for dev in others:
        remote(samp_msg, samp_all.at[me], samp_sem, dev).start()
    samp_all[me] = samp_msg[...]
    if more:
        fold_ref[...] = fold_hot(plan.low_out, plan.top_out)
    seg_col = to_col(seg_row)
    arrived(samp_all.at[rest], samp_sem)

    tile = (LANES, LANES)
    counts = []
    for part in range(ROWS // LANES):
        kblk = jnp.broadcast_to(key_col[part * LANES:(part + 1) * LANES], tile)

        def count(step, acc, kblk=kblk):
            for sub in range(8):
                row = (step * 8 + sub) * plan.share
                acc = acc + ones_where(sum(samp_all[row + no] for no in range(plan.share)) <= kblk)
            return acc

        counts.append(along_lanes(lax.fori_loop(0, plan.per // 8, count, jnp.zeros(tile, F32))))
    seen_col = jnp.concatenate(counts, axis=0)
    per_range = DEVS * plan.per // plan.ranges
    range_col = jnp.maximum(jnp.floor((seen_col - (DEVS // 2 + 1)) * (1.0 / per_range)), 0.0)
    range_row = to_row(range_col)
    slot_col = rank_col - along_lanes(ones_where(range_row < range_col))
    low_col = jnp.where(slot_col < BASE, range_col * BASE + slot_col, -1.0)
    low_row = to_row(low_col)
    top_col = jnp.where((slot_col >= BASE) & (slot_col < plan.full), range_col * more + (slot_col - BASE), -1.0)
    spill = ones_where(jnp.max(slot_col, axis=0, keepdims=True) >= plan.full)

    hot_low = hot(low_row == iota((plan.low_out, 1), 0).astype(F32))
    if more:
        hot_top = hot(to_row(top_col) == iota((plan.top_out, 1), 0).astype(F32))
    fetch.wait()
    piles = []
    for part in range(parts):
        start = part * cols
        packed0[part, :, :half] = dot(hot_low, pay_ref[:, start:start + half]).astype(BF16)
        if more:
            piles.append(stack(dot(hot_top, pay_ref[:, start:start + cols]).astype(BF16), chunks))
    if more:
        folded = dot(fold_ref[...], jnp.concatenate(piles, axis=1)).astype(BF16)
        for part in range(parts):
            packed0[part, :, half:] = folded[:, part * LANES:(part + 1) * LANES]

    def send_rows(devs, src, dst, sem):
        for dev in devs:
            remote(src.at[dev & (parts - 1), at16(dev >> plan.shift)], dst.at[at16(me)], sem, dev).start()

    send_rows(others[:EARLY], packed0, recv0, row_sem0)

    lane_val = lane_one // plan.full
    lane_slot = (lane_one % plan.full).astype(F32)
    vals = jnp.where(lane_val == 0, key_col, 1.0)
    vals = jnp.where(lane_val == 1, (seg_col >> 16).astype(F32), vals)
    vals = jnp.where(lane_val == 2, (seg_col & 65535).astype(F32), vals)
    vals = jnp.where((lane_slot == slot_col) & (lane_val < 4), vals, 0.0)
    range_b = jnp.broadcast_to(range_col, wide)
    for dst in range(plan.ranges):
        meta = along_sublanes(jnp.where(range_b == float(dst), vals, 0.0))
        meta_msg[dst] = jnp.where(lane_one == FLAG, spill, meta)
    for dev in others:
        remote(meta_msg.at[dev >> plan.shift], meta_all.at[me], meta_sem, dev).start()
    meta_all[me] = meta_msg[my_range]
    send_rows(others[EARLY:], packed0, recv0, row_sem0)

    for part in range(parts):
        start = part * cols + half
        packed1[part] = dot(hot_low, pay_ref[:, start:start + half]).astype(BF16)
    send_rows(others, packed1, recv1, row_sem1)
    recv0[at16(me)] = packed0[my_part, at16(my_range)]
    recv1[at16(me)] = packed1[my_part, at16(my_range)]
    arrived(meta_all.at[rest], meta_sem)

    low_tiles = plan.low // LANES
    tiles = plan.need // LANES
    each = LANES // BASE
    quarters = BASE // MORE
    sub = iota((LANES, 1), 0)
    diag = sub == lane_one

    def read_slots(got, slot):
        found = [along_lanes(jnp.where(lane_one == slot + no * plan.full, got, 0.0)) for no in range(4)]
        seg = (found[1].astype(I32) << 16) + found[2].astype(I32)
        return found[3] > 0.0, found[0], seg

    def keep(step, live, key, seg):
        rows = pl.ds(step * LANES, LANES)
        kcol_ref[rows] = jnp.broadcast_to(jnp.where(live, key, NEG), tile)
        scol_ref[rows] = jnp.broadcast_to(seg, tile)

    def to_lanes(spot, live, key, seg):
        return along_sublanes(jnp.where(spot, jnp.where(live, key, POS), 0.0)), along_sublanes(jnp.where(spot, seg, 0))

    top_keys, top_segs = [], []
    for step in range(low_tiles):
        got = meta_all[step * each:(step + 1) * each]
        got = jnp.broadcast_to(got, (each, BASE, LANES)).reshape(tile)
        slots = read_slots(got, sub & (BASE - 1))
        keep(step, *slots)
        krow_ref[step], srow_ref[step] = to_lanes(diag, *slots)
        if more:
            first = (step % quarters) * (LANES // quarters)
            spot = (lane_one == first + (sub >> 4) * MORE + (sub & (MORE - 1))) & ((sub & (BASE - 1)) < MORE)
            key, seg = to_lanes(spot, *read_slots(got, BASE + (sub & (MORE - 1))))
            top_keys.append(key)
            top_segs.append(seg)
    for no in range(tiles - low_tiles):
        step = low_tiles + no
        krow_ref[step] = sum(top_keys[no * quarters:(no + 1) * quarters])
        srow_ref[step] = sum(top_segs[no * quarters:(no + 1) * quarters])
        key = along_lanes(jnp.where(diag, jnp.broadcast_to(krow_ref[step], tile), 0.0))
        seg = along_lanes(jnp.where(diag, jnp.broadcast_to(srow_ref[step], tile), 0))
        keep(step, key < POS, key, seg)
    flags = jnp.max(jnp.where(lane_one == FLAG, meta_all[:, 0, :], 0.0), axis=0, keepdims=True)
    flag_ref[0, 0] = jnp.max(flags)

    def masks(step, carry):
        rows = pl.ds(pl.multiple_of(step * TALL, TALL), TALL)
        kcol = kcol_ref[rows]
        scol = scol_ref[rows]
        best = jnp.full((TALL, LANES), NEG, F32)
        for t in range(tiles):
            best = jnp.maximum(best, jnp.where((krow_ref[t] < kcol) & (srow_ref[t] != scol), krow_ref[t], NEG))
        bound = jnp.broadcast_to(jnp.max(best, axis=1, keepdims=True), best.shape)
        bcol_ref[rows] = bound
        for t in range(tiles):
            mask_ref[rows, t * LANES:(t + 1) * LANES] = hot((krow_ref[t] > bound) & (krow_ref[t] <= kcol))
        return carry

    lax.fori_loop(0, plan.need // TALL, masks, 0)

    krow = [krow_ref[t] for t in range(tiles)]
    srow = [srow_ref[t] for t in range(tiles)]

    def over(items, join, red):
        return red(functools.reduce(join, items), axis=1, keepdims=True)

    key_last = over([jnp.where(k < POS, k, NEG) for k in krow], jnp.maximum, jnp.max)
    key_first = over(krow, jnp.minimum, jnp.min)

    def pick(key):
        seg = over([jnp.where(k == key, s, 0) for k, s in zip(krow, srow)], jnp.add, jnp.sum)
        return seg, [(seg >> 16).astype(F32), (seg & 65535).astype(F32)]

    seg_last, last = pick(key_last)
    _, first = pick(key_first)
    cut = over([jnp.where((k < POS) & (s != seg_last), k, NEG) for k, s in zip(krow, srow)], jnp.maximum, jnp.max)
    tail_hot = jnp.concatenate([ones_where((k > cut) & (k < POS)) for k in krow], axis=1)
    tail_hot = jnp.broadcast_to(tail_hot, (BASE, plan.need)).astype(BF16)
    facts = jnp.zeros((1, LANES), F32)
    for no, val in enumerate(first + last + [ones_where(cut > NEG)]):
        facts = jnp.where(lane_one == no, val, facts)

    hot_low_ref[...] = hot(low_col == iota((1, plan.low_out), 1).astype(F32))
    if more:
        fold_ref[...] = unfold_hot(plan.low_out, plan.top_out)
        hot_top_ref[...] = hot(top_col == iota((1, plan.top_out), 1).astype(F32))

    def apply(mask, recv, no):
        total = dot(mask[:, :plan.low], recv[:, :half])
        return total + dot(mask[:, plan.low:], top_ref[:, no * half:(no + 1) * half]) if more else total

    def send_tail(msg, dst, sem):
        for step in range(1, plan.ranges):
            remote(msg, dst.at[my_range], sem, (me + step * parts) & (DEVS - 1)).start()
        dst[my_range] = msg[...]

    big = 256

    def products(recv, no):
        def step(blk, carry):
            rows = pl.ds(pl.multiple_of(blk * big, big), big)
            acc_ref[rows] = apply(mask_ref[rows], recv, no)
            return carry

        lax.fori_loop(0, plan.need // big, step, 0)

    arrived(recv0.at[most], row_sem0)
    piled = big // quarters
    if more:
        widen = unfold_hot(big, piled)
        for blk in range(plan.low // big):
            full = dot(widen, recv0[blk * big:(blk + 1) * big, half:]).astype(BF16)
            for c in range(chunks):
                top_ref[blk * piled:(blk + 1) * piled, c * LANES:(c + 1) * LANES] = full[c * piled:(c + 1) * piled]
    tail_msg0[:, :half] = apply(tail_hot, recv0, 0)[:1]
    tail_msg0[:, half:] = facts
    send_tail(tail_msg0, tail_all0, tail_sem0)
    products(recv0, 0)
    arrived(recv1.at[most], row_sem1)
    tail_msg1[...] = apply(tail_hot, recv1, 1)[:1]
    send_tail(tail_msg1, tail_all1, tail_sem1)
    tails0 = tail_all0.at[pl.ds(0, plan.ranges - 1)]
    tails1 = tail_all1.at[pl.ds(0, plan.ranges - 1)]
    arrived(tails0, tail_sem0)

    fact = [along_lanes(jnp.where(lane_one == no, tail_all0[:, 0, half:], 0.0)) for no in range(5)]
    range_no = iota((plan.ranges, 1), 0)
    before = range_no < my_range
    same_first = (fact[0] == first[0]) & (fact[1] == first[1])
    same_last = (fact[2] == first[0]) & (fact[3] == first[1])
    stop = before & ((fact[4] > 0.0) | jnp.logical_not(same_first))
    last_stop = jnp.max(jnp.where(stop, range_no, -1), axis=0, keepdims=True)
    linked = before & ((range_no > last_stop) | ((range_no == last_stop) & same_last))

    def finish(tails, no, sums):
        carry_in = along_sublanes(jnp.where(linked, tails[:, 0, :half], 0.0))

        def closed(rows):
            return (acc_ref[rows] + jnp.where(bcol_ref[rows][:, :1] == NEG, carry_in, 0.0)).astype(BF16)

        def step(blk, carry):
            rows = pl.ds(pl.multiple_of(blk * big, big), big)
            sums[rows, :half] = closed(rows)
            return carry

        lax.fori_loop(0, plan.low // big, step, 0)
        if more:
            top_done[:, no * half:(no + 1) * half] = closed(pl.ds(plan.low, plan.top))

    def send_back(src, dst, sem):
        for dev in others:
            remote(src.at[at16(dev)], dst.at[my_part, at16(my_range)], sem, dev).start()
        dst[my_part, at16(my_range)] = src[at16(me)]

    finish(tail_all0, 0, sums0)
    send_back(sums0, ret0, ret_sem0)

    products(recv1, 1)
    arrived(tails1, tail_sem1)
    finish(tail_all1, 1, sums1)
    if more:
        narrow = fold_hot(big, piled)
        for blk in range(plan.top // piled):
            pile = stack(top_done[blk * piled:(blk + 1) * piled], chunks)
            sums1[blk * big:(blk + 1) * big, half:] = dot(narrow, pile).astype(BF16)
    send_back(sums1, ret1, ret_sem1)

    arrived(recv1.at[most], ret_sem0)
    if not more:
        for part in range(parts):
            start = part * cols
            out_ref[:, start:start + half] = dot(hot_low_ref[...], ret0[part]).astype(BF16)
    else:
        for part in range(parts):
            back_ref[:, part * half:(part + 1) * half] = dot(hot_low_ref[...], ret0[part])
    arrived(recv0.at[most], ret_sem1)
    if more:
        piles = jnp.concatenate([ret1[part, :, half:] for part in range(parts)], axis=1)
        piles = dot(fold_ref[...], piles).astype(BF16)
    for part in range(parts):
        start = part * cols
        rows = dot(hot_low_ref[...], ret1[part, :, :half])
        if more:
            top_rows = jnp.concatenate([piles[c * plan.top_out:(c + 1) * plan.top_out, part * LANES:(part + 1) * LANES]
                                        for c in range(chunks)], axis=1)
            top_rows = dot(hot_top_ref[...], top_rows)
            rows = rows + top_rows[:, half:]
            out_ref[:, start:start + half] = (back_ref[:, part * half:(part + 1) * half] + top_rows[:, :half]).astype(BF16)
        out_ref[:, start + half:start + cols] = rows.astype(BF16)

    for like in (samp_all.at[rest], meta_all.at[rest], recv0.at[most], recv1.at[most], tails0, tails1, recv0.at[most],
                 recv1.at[most]):
        left(like)


def run(plan, call_id, keys, segs, payload):
    vmem = pl.BlockSpec(memory_space=pltpu.VMEM)
    shapes = [
        ((ROWS, WIDTH), BF16),
        ((1, LANES), F32),
        ((DEVS, 1, LANES), F32),
        ((plan.low_out, plan.low_out) if plan.more else (BASE, LANES), BF16),
        ((plan.parts, plan.low_out, plan.long), BF16),
        ((plan.parts, plan.low_out, plan.half), BF16),
        ((plan.low, plan.long), BF16),
        ((plan.low, plan.half), BF16),
        ((plan.ranges, 1, LANES), F32),
        ((DEVS, 1, LANES), F32),
        ((plan.need, plan.need), BF16),
        ((plan.need, LANES), F32),
        ((plan.need, LANES), I32),
        ((plan.need, LANES), F32),
        ((plan.need // LANES, 1, LANES), F32),
        ((plan.need // LANES, 1, LANES), I32),
        ((1, plan.half + LANES), F32),
        ((1, plan.half), F32),
        ((plan.ranges, 1, plan.half + LANES), F32),
        ((plan.ranges, 1, plan.half), F32),
        ((max(plan.top, BASE), plan.cols), BF16),
        ((plan.need, plan.half), F32),
        ((max(plan.top, BASE), plan.cols), BF16),
        ((plan.low, plan.half), BF16),
        ((plan.low, plan.long), BF16),
        ((plan.parts, plan.low_out, plan.half), BF16),
        ((plan.parts, plan.low_out, plan.long), BF16),
        ((ROWS, WIDTH // 2) if plan.more else (8, LANES), F32),
        ((ROWS, plan.low_out), BF16),
        ((ROWS, max(plan.top_out, LANES)), BF16),
    ]
    return pl.pallas_call(
        functools.partial(kernel, plan),
        out_shape=(jax.ShapeDtypeStruct((ROWS, WIDTH), BF16), jax.ShapeDtypeStruct((1, 1), F32)),
        in_specs=[vmem, vmem, pl.BlockSpec(memory_space=pl.ANY)],
        out_specs=(vmem, pl.BlockSpec(memory_space=pltpu.SMEM)),
        scratch_shapes=[pltpu.VMEM(*shape) for shape in shapes] + [pltpu.SemaphoreType.DMA] * 10,
        compiler_params=pltpu.CompilerParams(collective_id=call_id, has_side_effects=True, vmem_limit_bytes=62 << 20),
    )(keys, segs, payload)


def settle_kernel(src_ref, dst_ref):
    dst_ref[...] = src_ref[...]


def settle(done):
    block = pl.BlockSpec((ROWS // 4, WIDTH), lambda step: (step, 0))
    return pl.pallas_call(settle_kernel, out_shape=jax.ShapeDtypeStruct((ROWS, WIDTH), BF16), grid=(4,),
                          in_specs=[block], out_specs=block)(done)


def solution(mesh):
    def per_device(sort_keys, seg_ids, payload):
        args = (sort_keys.reshape(1, ROWS), seg_ids.reshape(1, ROWS), payload)
        out, flag = run(NARROW, 0, *args)
        return settle(lax.cond(flag[0, 0] > 0.0, lambda done: run(FULL, 1, *args)[0], lambda done: done, out))

    row_spec = P(('batch', 'group'))
    mat_spec = P(('batch', 'group'), None)
    return jax.shard_map(per_device, mesh=mesh, in_specs=(row_spec, row_spec, mat_spec),
                         out_specs=mat_spec, check_vma=False)
```

```python
import functools

import jax
import jax.numpy as jnp
from jax import lax
from jax.experimental import pallas as pl
from jax.experimental.pallas import tpu as pltpu
from jax.sharding import PartitionSpec as P

F32 = jnp.float32
BF16 = jnp.bfloat16
I32 = jnp.int32
NEG = float('-inf')
POS = float('inf')
MESH = pl.DeviceIdType.MESH

DEVS = 128
ROWS = 512
WIDTH = 2048
LANES = 128
BASE = 16
MORE = 4
FLAG = LANES - 1
TALL = 128
RING = 4


class Plan:
    def __init__(self, parts, more, stride):
        self.parts, self.more, self.stride = parts, more, stride
        self.shift = parts.bit_length() - 1
        self.ranges = DEVS // parts
        self.per = ROWS // stride
        self.share = LANES // self.per
        self.cols = WIDTH // parts
        self.half = self.cols // 2
        self.chunks = self.cols // LANES
        self.full = BASE + more
        self.extra = LANES if more else 0
        self.long = self.half + self.extra
        self.low = DEVS * BASE
        self.top = DEVS * more
        self.need = self.low + self.top
        self.low_out = self.ranges * BASE
        self.top_out = self.ranges * more


NARROW = Plan(4, MORE, BASE)
FULL = Plan(2, 0, 4)


def iota(shape, dim):
    return lax.broadcasted_iota(I32, shape, dim)


def ones_where(hit):
    return jnp.where(hit, 1.0, 0.0)


def hot(hit):
    return ones_where(hit).astype(BF16)


def dot(left, right):
    return jnp.dot(left, right, preferred_element_type=F32)


def along_sublanes(vals):
    return jnp.sum(vals, axis=0, keepdims=True)


def along_lanes(vals):
    return jnp.sum(vals, axis=1, keepdims=True)


def fold(to, groups):
    return ((to & (BASE - 1)) >> 2) * groups + (to >> 4) * MORE + (to & (MORE - 1))


def fold_hot(size, groups):
    return hot(fold(iota((size, 1), 0), groups) == iota((1, size), 1))


def unfold_hot(size, groups):
    return hot(iota((size, 1), 0) == fold(iota((1, size), 1), groups))


def stack(rows, chunks):
    return jnp.concatenate([rows[:, c * LANES:(c + 1) * LANES] for c in range(chunks)], axis=0)


def place(me, step):
    core, x, y, z = me & 1, (me >> 1) & (RING - 1), (me >> 3) & (RING - 1), me >> 5
    return (core + step) & 1, ((x + step) & (RING - 1)) << 1, ((y + step) & (RING - 1)) << 3, ((z + step) & (RING - 1)) << 5


def other_devices(me):
    places = [place(me, step) for step in range(RING)]
    found, starts = [], []

    def add(along_x, along_y, along_z, flip):
        found.append(places[along_z % RING][3] + places[along_y % RING][2] + places[along_x][1] + places[flip][0])

    for near in (True, False):
        for flip in range(2):
            starts.append(len(found))
            for along_z in range(RING):
                for along_y in range(RING):
                    if near:
                        add(1, along_y, along_z, flip)
                        add(3, along_y + 2, along_z + 2, flip)
                    else:
                        add(2, along_y + 2, along_z + 2, flip)
                        if along_y or along_z or flip:
                            add(0, along_y, along_z, flip)
    return found, starts


def kernel(plan, keys_ref, segs_ref, pay_hbm, out_hbm, flag_ref, pay_ref, samp_msg, samp_all, fold_ref, packed0, packed1,
           recv0, recv1, meta_msg, meta_all, mask_ref, kcol_ref, scol_ref, bcol_ref, krow_ref, srow_ref, tail_msg0,
           tail_msg1, tail_all0, tail_all1, top_ref, acc_ref, top_done, sums0, sums1, ret0, ret1, back_ref, hot_low_ref,
           hot_top_ref, pay_sem, send_sem, samp_sem, meta_sem, row_sem0, row_sem1, tail_sem0, tail_sem1, ret_sem0,
           ret_sem1, out_sem):
    parts, more, cols, half, chunks = plan.parts, plan.more, plan.cols, plan.half, plan.chunks
    me = lax.axis_index('group')
    my_range = me >> plan.shift
    my_part = me & (parts - 1)
    barrier = pltpu.get_barrier_semaphore()
    others, starts = other_devices(me)
    rest = pl.ds(0, DEVS - 1)
    most = pl.ds(0, plan.low - BASE)

    def remote(src, dst, recv_sem, dev):
        return pltpu.make_async_remote_copy(src_ref=src, dst_ref=dst, send_sem=send_sem, recv_sem=recv_sem,
                                            device_id={'group': dev}, device_id_type=MESH)

    def arrived(like, sem):
        remote(like, like, sem, others[0]).wait_recv()

    def left(like):
        remote(like, like, ret_sem0, others[0]).wait_send()

    def at16(no):
        return pl.ds(pl.multiple_of(no * BASE, BASE), BASE)

    for dev in others:
        pl.semaphore_signal(barrier, inc=1, device_id={'group': dev}, device_id_type=MESH)
    fetch = pltpu.make_async_copy(pay_hbm, pay_ref, pay_sem)
    fetch.start()

    key_row = keys_ref[...]
    seg_row = segs_ref[...]
    square = (ROWS, ROWS)
    eye = iota(square, 0) == iota(square, 1)

    def to_col(row):
        return along_lanes(jnp.where(eye, jnp.broadcast_to(row, square), 0))

    def to_row(col):
        return along_sublanes(jnp.where(eye, jnp.broadcast_to(col, square), 0))

    key_col = to_col(key_row)
    rank_col = along_lanes(ones_where(key_row < key_col))
    wide = (ROWS, LANES)
    lane_one = iota((1, LANES), 1)
    chosen = ((lane_one - (me & (plan.share - 1)) * plan.per) * plan.stride).astype(F32)
    samp_msg[...] = along_sublanes(jnp.where(rank_col == chosen, jnp.broadcast_to(key_col, wide), 0.0))
    pl.semaphore_wait(barrier, DEVS - 1)

    for dev in others:
        remote(samp_msg, samp_all.at[me], samp_sem, dev).start()
    samp_all[me] = samp_msg[...]
    if more:
        fold_ref[...] = fold_hot(plan.low_out, plan.top_out)
    seg_col = to_col(seg_row)
    arrived(samp_all.at[rest], samp_sem)

    tile = (LANES, LANES)
    counts = []
    for part in range(ROWS // LANES):
        kblk = jnp.broadcast_to(key_col[part * LANES:(part + 1) * LANES], tile)

        def count(step, acc, kblk=kblk):
            for sub in range(8):
                row = (step * 8 + sub) * plan.share
                acc = acc + ones_where(sum(samp_all[row + no] for no in range(plan.share)) <= kblk)
            return acc

        counts.append(along_lanes(lax.fori_loop(0, plan.per // 8, count, jnp.zeros(tile, F32))))
    seen_col = jnp.concatenate(counts, axis=0)
    per_range = DEVS * plan.per // plan.ranges
    range_col = jnp.maximum(jnp.floor((seen_col - (DEVS // 2 + 1)) * (1.0 / per_range)), 0.0)
    range_row = to_row(range_col)
    slot_col = rank_col - along_lanes(ones_where(range_row < range_col))
    low_col = jnp.where(slot_col < BASE, range_col * BASE + slot_col, -1.0)
    low_row = to_row(low_col)
    top_col = jnp.where((slot_col >= BASE) & (slot_col < plan.full), range_col * more + (slot_col - BASE), -1.0)
    spill = ones_where(jnp.max(slot_col, axis=0, keepdims=True) >= plan.full)

    hot_low = hot(low_row == iota((plan.low_out, 1), 0).astype(F32))
    if more:
        hot_top = hot(to_row(top_col) == iota((plan.top_out, 1), 0).astype(F32))
    fetch.wait()
    turns = [others[no] & (parts - 1) for no in starts]

    def pack(part, dst, first):
        start = part * cols + first
        rows = pay_ref[:, pl.ds(pl.multiple_of(start, half), half)]
        dst[part, :, :half] = dot(hot_low, rows).astype(BF16)

    def pack_top(part):
        rows = dot(hot_top, pay_ref[:, pl.ds(pl.multiple_of(part * cols, cols), cols)]).astype(BF16)
        packed0[part, :, half:] = dot(fold_ref[...], stack(rows, chunks)).astype(BF16)

    def pack_first(part):
        pack(part, packed0, 0)
        if more:
            pack_top(part)

    def send_rows(no, src, dst, sem):
        for dev in others[starts[no]:(starts + [DEVS - 1])[no + 1]]:
            remote(src.at[dev & (parts - 1), at16(dev >> plan.shift)], dst.at[at16(me)], sem, dev).start()

    pack_first(turns[0])
    send_rows(0, packed0, recv0, row_sem0)

    lane_val = lane_one // plan.full
    lane_slot = (lane_one % plan.full).astype(F32)
    vals = jnp.where(lane_val == 0, key_col, (seg_col & 65535).astype(F32))
    vals = jnp.where(lane_val == 1, (seg_col >> 16).astype(F32), vals)
    vals = jnp.where((lane_slot == slot_col) & (lane_val < 3), vals, POS)
    range_b = jnp.broadcast_to(range_col, wide)
    for dst in range(plan.ranges):
        meta = jnp.min(jnp.where(range_b == float(dst), vals, POS), axis=0, keepdims=True)
        meta_msg[dst] = jnp.where(lane_one == FLAG, spill, meta)
    for dev in others:
        remote(meta_msg.at[dev >> plan.shift], meta_all.at[me], meta_sem, dev).start()
    meta_all[me] = meta_msg[my_range]
    for no in range(1, len(turns)):
        if no < parts:
            pack_first(turns[no])
        send_rows(no, packed0, recv0, row_sem0)

    for no in range(len(turns)):
        if no < parts:
            pack(turns[no], packed1, half)
        send_rows(no, packed1, recv1, row_sem1)
    recv0[at16(me)] = packed0[my_part, at16(my_range)]
    recv1[at16(me)] = packed1[my_part, at16(my_range)]
    arrived(meta_all.at[rest], meta_sem)

    low_tiles = plan.low // LANES
    tiles = plan.need // LANES
    each = LANES // BASE
    quarters = BASE // MORE
    sub = iota((LANES, 1), 0)
    diag = sub == lane_one

    def read_slots(got, slot):
        found = [along_lanes(jnp.where(lane_one == slot + no * plan.full, got, 0.0)) for no in range(3)]
        live = found[0] < POS
        high, low = [jnp.where(live, val, 0.0).astype(I32) for val in found[1:]]
        return live, found[0], (high << 16) + low

    def keep(step, live, key, seg):
        rows = pl.ds(step * LANES, LANES)
        kcol_ref[rows] = jnp.broadcast_to(jnp.where(live, key, NEG), tile)
        scol_ref[rows] = jnp.broadcast_to(seg, tile)

    def to_lanes(step, spot, key, seg):
        krow_ref[step] = along_sublanes(jnp.where(spot, key, 0.0))
        srow_ref[step] = along_sublanes(jnp.where(spot, seg, 0))

    mixed = []
    for step in range(low_tiles):
        got = meta_all[step * each:(step + 1) * each]
        got = jnp.broadcast_to(got, (each, BASE, LANES)).reshape(tile)
        live, key, seg = read_slots(got, sub & (BASE - 1))
        keep(step, live, key, seg)
        to_lanes(step, diag, key, seg)
        if more:
            turn = step % quarters
            merged = jnp.where(((sub & (BASE - 1)) >> 2) == turn, got, merged if turn else 0.0)
            if turn == quarters - 1:
                mixed.append(merged)
    for no, merged in enumerate(mixed):
        step = low_tiles + no
        _, key, seg = read_slots(merged, BASE + (sub & (MORE - 1)))
        spot = lane_one == (((sub & (BASE - 1)) >> 2) * each + (sub >> 4)) * MORE + (sub & (MORE - 1))
        to_lanes(step, spot, key, seg)
        key = along_lanes(jnp.where(diag, jnp.broadcast_to(krow_ref[step], tile), 0.0))
        seg = along_lanes(jnp.where(diag, jnp.broadcast_to(srow_ref[step], tile), 0))
        keep(step, key < POS, key, seg)
    flags = jnp.max(jnp.where(lane_one == FLAG, meta_all[:, 0, :], 0.0), axis=0, keepdims=True)
    flag_ref[0, 0] = jnp.max(flags)

    def masks(step, carry):
        rows = pl.ds(pl.multiple_of(step * TALL, TALL), TALL)
        kcol = kcol_ref[rows]
        scol = scol_ref[rows]
        best = jnp.full((TALL, LANES), NEG, F32)
        for t in range(tiles):
            best = jnp.maximum(best, jnp.where((krow_ref[t] < kcol) & (srow_ref[t] != scol), krow_ref[t], NEG))
        bound = jnp.broadcast_to(jnp.max(best, axis=1, keepdims=True), best.shape)
        bcol_ref[rows] = bound
        for t in range(tiles):
            mask_ref[rows, t * LANES:(t + 1) * LANES] = hot((krow_ref[t] > bound) & (krow_ref[t] <= kcol))
        return carry

    lax.fori_loop(0, plan.need // TALL, masks, 0)

    krow = [krow_ref[t] for t in range(tiles)]
    srow = [srow_ref[t] for t in range(tiles)]

    def over(items, join, red):
        return red(functools.reduce(join, items), axis=1, keepdims=True)

    key_last = over([jnp.where(k < POS, k, NEG) for k in krow], jnp.maximum, jnp.max)
    key_first = over(krow, jnp.minimum, jnp.min)

    def pick(key):
        seg = over([jnp.where(k == key, s, 0) for k, s in zip(krow, srow)], jnp.add, jnp.sum)
        return seg, [(seg >> 16).astype(F32), (seg & 65535).astype(F32)]

    seg_last, last = pick(key_last)
    _, first = pick(key_first)
    cut = over([jnp.where((k < POS) & (s != seg_last), k, NEG) for k, s in zip(krow, srow)], jnp.maximum, jnp.max)
    tail_hot = jnp.concatenate([ones_where((k > cut) & (k < POS)) for k in krow], axis=1)
    tail_hot = jnp.broadcast_to(tail_hot, (BASE, plan.need)).astype(BF16)
    facts = jnp.zeros((1, LANES), F32)
    for no, val in enumerate(first + last + [ones_where(cut > NEG)]):
        facts = jnp.where(lane_one == no, val, facts)

    def apply(mask, recv, no):
        total = dot(mask[:, :plan.low], recv[:, :half])
        return total + dot(mask[:, plan.low:], top_ref[:, no * half:(no + 1) * half]) if more else total

    def send_tail(msg, dst, sem):
        for step in range(1, plan.ranges):
            remote(msg, dst.at[my_range], sem, (me + step * parts) & (DEVS - 1)).start()
        dst[my_range] = msg[...]

    big = 256

    def products(recv, no):
        def step(blk, carry):
            rows = pl.ds(pl.multiple_of(blk * big, big), big)
            acc_ref[rows] = apply(mask_ref[rows], recv, no)
            return carry

        lax.fori_loop(0, plan.need // big, step, 0)

    arrived(recv0.at[most], row_sem0)
    piled = big // quarters
    if more:
        widen = unfold_hot(big, piled)
        for blk in range(plan.low // big):
            full = dot(widen, recv0[blk * big:(blk + 1) * big, half:]).astype(BF16)
            for c in range(chunks):
                top_ref[blk * piled:(blk + 1) * piled, c * LANES:(c + 1) * LANES] = full[c * piled:(c + 1) * piled]
    tail_msg0[:, :half] = apply(tail_hot, recv0, 0)[:1]
    tail_msg0[:, half:] = facts
    send_tail(tail_msg0, tail_all0, tail_sem0)
    products(recv0, 0)
    arrived(recv1.at[most], row_sem1)
    tail_msg1[...] = apply(tail_hot, recv1, 1)[:1]
    send_tail(tail_msg1, tail_all1, tail_sem1)
    tails0 = tail_all0.at[pl.ds(0, plan.ranges - 1)]
    tails1 = tail_all1.at[pl.ds(0, plan.ranges - 1)]
    arrived(tails0, tail_sem0)

    fact = [along_lanes(jnp.where(lane_one == no, tail_all0[:, 0, half:], 0.0)) for no in range(5)]
    range_no = iota((plan.ranges, 1), 0)
    before = range_no < my_range
    same_first = (fact[0] == first[0]) & (fact[1] == first[1])
    same_last = (fact[2] == first[0]) & (fact[3] == first[1])
    stop = before & ((fact[4] > 0.0) | jnp.logical_not(same_first))
    last_stop = jnp.max(jnp.where(stop, range_no, -1), axis=0, keepdims=True)
    linked = before & ((range_no > last_stop) | ((range_no == last_stop) & same_last))

    def finish(tails, no, sums):
        carry_in = along_sublanes(jnp.where(linked, tails[:, 0, :half], 0.0))

        def closed(rows):
            return (acc_ref[rows] + jnp.where(bcol_ref[rows][:, :1] == NEG, carry_in, 0.0)).astype(BF16)

        def step(blk, carry):
            rows = pl.ds(pl.multiple_of(blk * big, big), big)
            sums[rows, :half] = closed(rows)
            return carry

        lax.fori_loop(0, plan.low // big, step, 0)
        if more:
            top_done[:, no * half:(no + 1) * half] = closed(pl.ds(plan.low, plan.top))

    def send_back(src, dst, sem):
        for dev in others:
            remote(src.at[at16(dev)], dst.at[my_part, at16(my_range)], sem, dev).start()
        dst[my_part, at16(my_range)] = src[at16(me)]

    finish(tail_all0, 0, sums0)
    send_back(sums0, ret0, ret_sem0)

    products(recv1, 1)
    arrived(tails1, tail_sem1)
    finish(tail_all1, 1, sums1)
    if more:
        narrow = fold_hot(big, piled)
        for blk in range(plan.top // piled):
            pile = stack(top_done[blk * piled:(blk + 1) * piled], chunks)
            sums1[blk * big:(blk + 1) * big, half:] = dot(narrow, pile).astype(BF16)
    send_back(sums1, ret1, ret_sem1)

    hot_low_ref[...] = hot(low_col == iota((1, plan.low_out), 1).astype(F32))
    if more:
        fold_ref[...] = unfold_hot(plan.low_out, plan.top_out)
        hot_top_ref[...] = hot(top_col == iota((1, plan.top_out), 1).astype(F32))

    arrived(recv1.at[most], ret_sem0)
    if not more:
        for part in range(parts):
            start = part * cols
            pay_ref[:, start:start + half] = dot(hot_low_ref[...], ret0[part]).astype(BF16)
    else:
        for part in range(parts):
            back_ref[:, part * half:(part + 1) * half] = dot(hot_low_ref[...], ret0[part])
    arrived(recv0.at[most], ret_sem1)
    results = []
    if more:
        piles = jnp.concatenate([ret1[part, :, half:] for part in range(parts)], axis=1)
        piles = dot(fold_ref[...], piles).astype(BF16)
    for part in range(parts):
        start = part * cols
        rows = dot(hot_low_ref[...], ret1[part, :, :half])
        if more:
            top_rows = jnp.concatenate([piles[c * plan.top_out:(c + 1) * plan.top_out, part * LANES:(part + 1) * LANES]
                                        for c in range(chunks)], axis=1)
            top_rows = dot(hot_top_ref[...], top_rows)
            rows = rows + top_rows[:, half:]
            pay_ref[:, start:start + half] = (back_ref[:, part * half:(part + 1) * half] + top_rows[:, :half]).astype(BF16)
        pay_ref[:, start + half:start + cols] = rows.astype(BF16)
        here = pl.ds(start, cols)
        copy = pltpu.make_async_copy(pay_ref.at[:, here], out_hbm.at[:, here], out_sem.at[part])
        copy.start()
        results.append(copy)

    for copy in results:
        copy.wait()

    for like in (samp_all.at[rest], meta_all.at[rest], recv0.at[most], recv1.at[most], tails0, tails1, recv0.at[most],
                 recv1.at[most]):
        left(like)


def run(plan, call_id, keys, segs, payload):
    vmem = pl.BlockSpec(memory_space=pltpu.VMEM)
    shapes = [
        ((ROWS, WIDTH), BF16),
        ((1, LANES), F32),
        ((DEVS, 1, LANES), F32),
        ((plan.low_out, plan.low_out) if plan.more else (BASE, LANES), BF16),
        ((plan.parts, plan.low_out, plan.long), BF16),
        ((plan.parts, plan.low_out, plan.half), BF16),
        ((plan.low, plan.long), BF16),
        ((plan.low, plan.half), BF16),
        ((plan.ranges, 1, LANES), F32),
        ((DEVS, 1, LANES), F32),
        ((plan.need, plan.need), BF16),
        ((plan.need, LANES), F32),
        ((plan.need, LANES), I32),
        ((plan.need, LANES), F32),
        ((plan.need // LANES, 1, LANES), F32),
        ((plan.need // LANES, 1, LANES), I32),
        ((1, plan.half + LANES), F32),
        ((1, plan.half), F32),
        ((plan.ranges, 1, plan.half + LANES), F32),
        ((plan.ranges, 1, plan.half), F32),
        ((max(plan.top, BASE), plan.cols), BF16),
        ((plan.need, plan.half), F32),
        ((max(plan.top, BASE), plan.cols), BF16),
        ((plan.low, plan.half), BF16),
        ((plan.low, plan.long), BF16),
        ((plan.parts, plan.low_out, plan.half), BF16),
        ((plan.parts, plan.low_out, plan.long), BF16),
        ((ROWS, WIDTH // 2) if plan.more else (8, LANES), F32),
        ((ROWS, plan.low_out), BF16),
        ((ROWS, max(plan.top_out, LANES)), BF16),
    ]
    return pl.pallas_call(
        functools.partial(kernel, plan),
        out_shape=(jax.ShapeDtypeStruct((ROWS, WIDTH), BF16), jax.ShapeDtypeStruct((1, 1), F32)),
        in_specs=[vmem, vmem, pl.BlockSpec(memory_space=pl.ANY)],
        out_specs=(pl.BlockSpec(memory_space=pl.ANY), pl.BlockSpec(memory_space=pltpu.SMEM)),
        scratch_shapes=[pltpu.VMEM(*shape) for shape in shapes] + [pltpu.SemaphoreType.DMA] * 10
        + [pltpu.SemaphoreType.DMA((plan.parts,))],
        compiler_params=pltpu.CompilerParams(collective_id=call_id, has_side_effects=True, vmem_limit_bytes=62 << 20),
    )(keys, segs, payload)


def settle_kernel(src_ref, dst_ref, buf, in_sem, out_sem):
    count = in_sem.shape[0]
    tall = ROWS // count
    rows = [pl.ds(no * tall, tall) for no in range(count)]
    into = [pltpu.make_async_copy(src_ref.at[row], buf.at[row], in_sem.at[no]) for no, row in enumerate(rows)]
    out = [pltpu.make_async_copy(buf.at[row], dst_ref.at[row], out_sem.at[no]) for no, row in enumerate(rows)]
    for copy in into:
        copy.start()
    for no in range(count):
        into[no].wait()
        out[no].start()
    for copy in out:
        copy.wait()


def settle(done):
    here = pl.BlockSpec(memory_space=pl.ANY)
    dma = pltpu.SemaphoreType.DMA((4,))
    return pl.pallas_call(settle_kernel, out_shape=jax.ShapeDtypeStruct((ROWS, WIDTH), BF16), in_specs=[here],
                          out_specs=here, scratch_shapes=[pltpu.VMEM((ROWS, WIDTH), BF16), dma, dma])(done)


def solution(mesh):
    def per_device(sort_keys, seg_ids, payload):
        args = (sort_keys.reshape(1, ROWS), seg_ids.reshape(1, ROWS), payload)
        out, flag = run(NARROW, 0, *args)
        return settle(lax.cond(flag[0, 0] > 0.0, lambda done: run(FULL, 1, *args)[0], lambda done: done, out))

    row_spec = P(('batch', 'group'))
    mat_spec = P(('batch', 'group'), None)
    return jax.shard_map(per_device, mesh=mesh, in_specs=(row_spec, row_spec, mat_spec),
                         out_specs=mat_spec, check_vma=False)
```

```python
import functools

import jax
import jax.numpy as jnp
from jax import lax
from jax.experimental import pallas as pl
from jax.experimental.pallas import tpu as pltpu
from jax.sharding import PartitionSpec as P

F32 = jnp.float32
BF16 = jnp.bfloat16
I32 = jnp.int32
NEG = float('-inf')
POS = float('inf')
MESH = pl.DeviceIdType.MESH

DEVS = 128
ROWS = 512
WIDTH = 2048
LANES = 128
BASE = 16
MORE = 4
FLAG = LANES - 1
TALL = 256
RING = 4


class Plan:
    def __init__(self, parts, more, stride):
        self.parts, self.more, self.stride = parts, more, stride
        self.shift = parts.bit_length() - 1
        self.ranges = DEVS // parts
        self.per = ROWS // stride
        self.share = LANES // self.per
        self.cols = WIDTH // parts
        self.half = self.cols // 2
        self.chunks = self.cols // LANES
        self.full = BASE + more
        self.extra = LANES if more else 0
        self.long = self.half + self.extra
        self.low = DEVS * BASE
        self.top = DEVS * more
        self.need = self.low + self.top
        self.low_out = self.ranges * BASE
        self.top_out = self.ranges * more


NARROW = Plan(4, MORE, BASE)
FULL = Plan(2, 0, 4)


def iota(shape, dim):
    return lax.broadcasted_iota(I32, shape, dim)


def ones_where(hit):
    return jnp.where(hit, 1.0, 0.0)


def hot(hit):
    return ones_where(hit).astype(BF16)


def dot(left, right):
    return jnp.dot(left, right, preferred_element_type=F32)


def along_sublanes(vals):
    return jnp.sum(vals, axis=0, keepdims=True)


def along_lanes(vals):
    return jnp.sum(vals, axis=1, keepdims=True)


def fold(to, groups):
    return ((to & (BASE - 1)) >> 2) * groups + (to >> 4) * MORE + (to & (MORE - 1))


def fold_hot(size, groups):
    return hot(fold(iota((size, 1), 0), groups) == iota((1, size), 1))


def unfold_hot(size, groups):
    return hot(iota((size, 1), 0) == fold(iota((1, size), 1), groups))


def stack(rows, chunks):
    return jnp.concatenate([rows[:, c * LANES:(c + 1) * LANES] for c in range(chunks)], axis=0)


def place(me, step):
    core, x, y, z = me & 1, (me >> 1) & (RING - 1), (me >> 3) & (RING - 1), me >> 5
    return (core + step) & 1, ((x + step) & (RING - 1)) << 1, ((y + step) & (RING - 1)) << 3, ((z + step) & (RING - 1)) << 5


def other_devices(me):
    places = [place(me, step) for step in range(RING)]
    found, starts = [], []

    def add(along_x, along_y, along_z, flip):
        found.append(places[along_z % RING][3] + places[along_y % RING][2] + places[along_x][1] + places[flip][0])

    for near in (True, False):
        for flip in range(2):
            starts.append(len(found))
            for along_z in range(RING):
                for along_y in range(RING):
                    if near:
                        add(1, along_y, along_z, flip)
                        add(3, along_y + 2, along_z + 2, flip)
                    else:
                        add(2, along_y + 2, along_z + 2, flip)
                        if along_y or along_z or flip:
                            add(0, along_y, along_z, flip)
    return found, starts


def kernel(plan, keys_ref, segs_ref, pay_hbm, out_hbm, flag_ref, pay_ref, samp_msg, samp_all, fold_ref, packed0, packed1,
           recv0, recv1, meta_msg, meta_all, mask_ref, kcol_ref, scol_ref, bcol_ref, krow_ref, srow_ref, tail_msg0,
           tail_msg1, tail_all0, tail_all1, top_ref, acc_ref, top_done, sums0, sums1, ret0, ret1, back_ref, hot_low_ref,
           hot_top_ref, pay_sem, send_sem, samp_sem, meta_sem, row_sem0, row_sem1, tail_sem0, tail_sem1, ret_sem0,
           ret_sem1, out_sem):
    parts, more, cols, half, chunks = plan.parts, plan.more, plan.cols, plan.half, plan.chunks
    me = lax.axis_index('group')
    my_range = me >> plan.shift
    my_part = me & (parts - 1)
    barrier = pltpu.get_barrier_semaphore()
    others, starts = other_devices(me)
    rest = pl.ds(0, DEVS - 1)
    most = pl.ds(0, plan.low - BASE)

    def remote(src, dst, recv_sem, dev):
        return pltpu.make_async_remote_copy(src_ref=src, dst_ref=dst, send_sem=send_sem, recv_sem=recv_sem,
                                            device_id={'group': dev}, device_id_type=MESH)

    def arrived(like, sem):
        remote(like, like, sem, others[0]).wait_recv()

    def left(like):
        remote(like, like, ret_sem0, others[0]).wait_send()

    def at16(no):
        return pl.ds(pl.multiple_of(no * BASE, BASE), BASE)

    for dev in others:
        pl.semaphore_signal(barrier, inc=1, device_id={'group': dev}, device_id_type=MESH)
    fetch = pltpu.make_async_copy(pay_hbm, pay_ref, pay_sem)
    fetch.start()

    key_row = keys_ref[...]
    seg_row = segs_ref[...]
    square = (ROWS, ROWS)
    eye = iota(square, 0) == iota(square, 1)

    def to_col(row):
        return along_lanes(jnp.where(eye, jnp.broadcast_to(row, square), 0))

    def to_row(col):
        return along_sublanes(jnp.where(eye, jnp.broadcast_to(col, square), 0))

    key_col = to_col(key_row)
    rank_col = along_lanes(ones_where(key_row < key_col))
    wide = (ROWS, LANES)
    lane_one = iota((1, LANES), 1)
    chosen = ((lane_one - (me & (plan.share - 1)) * plan.per) * plan.stride).astype(F32)
    samp_msg[...] = along_sublanes(jnp.where(rank_col == chosen, jnp.broadcast_to(key_col, wide), 0.0))
    pl.semaphore_wait(barrier, DEVS - 1)

    for dev in others:
        remote(samp_msg, samp_all.at[me], samp_sem, dev).start()
    samp_all[me] = samp_msg[...]
    if more:
        fold_ref[...] = fold_hot(plan.low_out, plan.top_out)
    seg_col = to_col(seg_row)
    arrived(samp_all.at[rest], samp_sem)

    tile = (LANES, LANES)
    counts = []
    for part in range(ROWS // LANES):
        kblk = jnp.broadcast_to(key_col[part * LANES:(part + 1) * LANES], tile)

        def count(step, acc, kblk=kblk):
            for sub in range(8):
                row = (step * 8 + sub) * plan.share
                acc = acc + ones_where(sum(samp_all[row + no] for no in range(plan.share)) <= kblk)
            return acc

        counts.append(along_lanes(lax.fori_loop(0, plan.per // 8, count, jnp.zeros(tile, F32))))
    seen_col = jnp.concatenate(counts, axis=0)
    per_range = DEVS * plan.per // plan.ranges
    range_col = jnp.maximum(jnp.floor((seen_col - (DEVS // 2 + 1)) * (1.0 / per_range)), 0.0)
    range_row = to_row(range_col)
    slot_col = rank_col - along_lanes(ones_where(range_row < range_col))
    low_col = jnp.where(slot_col < BASE, range_col * BASE + slot_col, -1.0)
    low_row = to_row(low_col)
    top_col = jnp.where((slot_col >= BASE) & (slot_col < plan.full), range_col * more + (slot_col - BASE), -1.0)
    spill = ones_where(jnp.max(slot_col, axis=0, keepdims=True) >= plan.full)

    hot_low = hot(low_row == iota((plan.low_out, 1), 0).astype(F32))
    if more:
        hot_top = hot(to_row(top_col) == iota((plan.top_out, 1), 0).astype(F32))
    fetch.wait()
    turns = [others[no] & (parts - 1) for no in starts]

    def pack(part, dst, first):
        start = part * cols + first
        rows = pay_ref[:, pl.ds(pl.multiple_of(start, half), half)]
        dst[part, :, :half] = dot(hot_low, rows).astype(BF16)

    def pack_top(part):
        rows = dot(hot_top, pay_ref[:, pl.ds(pl.multiple_of(part * cols, cols), cols)]).astype(BF16)
        packed0[part, :, half:] = dot(fold_ref[...], stack(rows, chunks)).astype(BF16)

    def pack_first(part):
        pack(part, packed0, 0)
        if more:
            pack_top(part)

    def send_rows(no, src, dst, sem):
        for dev in others[starts[no]:(starts + [DEVS - 1])[no + 1]]:
            remote(src.at[dev & (parts - 1), at16(dev >> plan.shift)], dst.at[at16(me)], sem, dev).start()

    pack_first(turns[0])
    send_rows(0, packed0, recv0, row_sem0)

    lane_val = lane_one // plan.full
    lane_slot = (lane_one % plan.full).astype(F32)
    vals = jnp.where(lane_val == 0, key_col, (seg_col & 65535).astype(F32))
    vals = jnp.where(lane_val == 1, (seg_col >> 16).astype(F32), vals)
    vals = jnp.where((lane_slot == slot_col) & (lane_val < 3), vals, POS)
    range_b = jnp.broadcast_to(range_col, wide)
    for dst in range(plan.ranges):
        meta = jnp.min(jnp.where(range_b == float(dst), vals, POS), axis=0, keepdims=True)
        meta_msg[dst] = jnp.where(lane_one == FLAG, spill, meta)
    for dev in others:
        remote(meta_msg.at[dev >> plan.shift], meta_all.at[me], meta_sem, dev).start()
    meta_all[me] = meta_msg[my_range]
    for no in range(1, len(turns)):
        if no < parts:
            pack_first(turns[no])
        send_rows(no, packed0, recv0, row_sem0)

    for no in range(len(turns)):
        if no < parts:
            pack(turns[no], packed1, half)
        send_rows(no, packed1, recv1, row_sem1)
    recv0[at16(me)] = packed0[my_part, at16(my_range)]
    recv1[at16(me)] = packed1[my_part, at16(my_range)]
    arrived(meta_all.at[rest], meta_sem)

    low_tiles = plan.low // LANES
    tiles = plan.need // LANES
    each = LANES // BASE
    quarters = BASE // MORE
    sub = iota((LANES, 1), 0)
    diag = sub == lane_one

    def read_slots(got, slot):
        found = [along_lanes(jnp.where(lane_one == slot + no * plan.full, got, 0.0)) for no in range(3)]
        live = found[0] < POS
        high, low = [jnp.where(live, val, 0.0).astype(I32) for val in found[1:]]
        return live, found[0], (high << 16) + low

    def keep(step, live, key, seg):
        rows = pl.ds(step * LANES, LANES)
        kcol_ref[rows] = jnp.broadcast_to(jnp.where(live, key, NEG), tile)
        scol_ref[rows] = jnp.broadcast_to(seg, tile)

    def to_lanes(step, spot, key, seg):
        krow_ref[step] = along_sublanes(jnp.where(spot, key, 0.0))
        srow_ref[step] = along_sublanes(jnp.where(spot, seg, 0))

    mixed = []
    for step in range(low_tiles):
        got = meta_all[step * each:(step + 1) * each]
        got = jnp.broadcast_to(got, (each, BASE, LANES)).reshape(tile)
        live, key, seg = read_slots(got, sub & (BASE - 1))
        keep(step, live, key, seg)
        to_lanes(step, diag, key, seg)
        if more:
            turn = step % quarters
            merged = jnp.where(((sub & (BASE - 1)) >> 2) == turn, got, merged if turn else 0.0)
            if turn == quarters - 1:
                mixed.append(merged)
    for no, merged in enumerate(mixed):
        step = low_tiles + no
        _, key, seg = read_slots(merged, BASE + (sub & (MORE - 1)))
        spot = lane_one == (((sub & (BASE - 1)) >> 2) * each + (sub >> 4)) * MORE + (sub & (MORE - 1))
        to_lanes(step, spot, key, seg)
        key = along_lanes(jnp.where(diag, jnp.broadcast_to(krow_ref[step], tile), 0.0))
        seg = along_lanes(jnp.where(diag, jnp.broadcast_to(srow_ref[step], tile), 0))
        keep(step, key < POS, key, seg)
    flags = jnp.max(jnp.where(lane_one == FLAG, meta_all[:, 0, :], 0.0), axis=0, keepdims=True)
    flag_ref[0, 0] = jnp.max(flags)

    def masks(step, carry):
        rows = pl.ds(pl.multiple_of(step * TALL, TALL), TALL)
        kcol = kcol_ref[rows]
        scol = scol_ref[rows]
        best = jnp.full((TALL, LANES), NEG, F32)
        for t in range(tiles):
            best = jnp.maximum(best, jnp.where((krow_ref[t] < kcol) & (srow_ref[t] != scol), krow_ref[t], NEG))
        bound = jnp.broadcast_to(jnp.max(best, axis=1, keepdims=True), best.shape)
        bcol_ref[rows] = bound
        for t in range(tiles):
            mask_ref[rows, t * LANES:(t + 1) * LANES] = hot((krow_ref[t] > bound) & (krow_ref[t] <= kcol))
        return carry

    lax.fori_loop(0, plan.need // TALL, masks, 0)

    krow = [krow_ref[t] for t in range(tiles)]
    srow = [srow_ref[t] for t in range(tiles)]

    def over(items, join, red):
        return red(functools.reduce(join, items), axis=1, keepdims=True)

    key_last = over([jnp.where(k < POS, k, NEG) for k in krow], jnp.maximum, jnp.max)
    key_first = over(krow, jnp.minimum, jnp.min)

    def pick(key):
        seg = over([jnp.where(k == key, s, 0) for k, s in zip(krow, srow)], jnp.add, jnp.sum)
        return seg, [(seg >> 16).astype(F32), (seg & 65535).astype(F32)]

    seg_last, last = pick(key_last)
    _, first = pick(key_first)
    cut = over([jnp.where((k < POS) & (s != seg_last), k, NEG) for k, s in zip(krow, srow)], jnp.maximum, jnp.max)
    tail_hot = jnp.concatenate([ones_where((k > cut) & (k < POS)) for k in krow], axis=1)
    tail_hot = jnp.broadcast_to(tail_hot, (BASE, plan.need)).astype(BF16)
    facts = jnp.zeros((1, LANES), F32)
    for no, val in enumerate(first + last + [ones_where(cut > NEG)]):
        facts = jnp.where(lane_one == no, val, facts)

    def apply(mask, recv, no):
        total = dot(mask[:, :plan.low], recv[:, :half])
        return total + dot(mask[:, plan.low:], top_ref[:, no * half:(no + 1) * half]) if more else total

    def send_tail(msg, dst, sem):
        for step in range(1, plan.ranges):
            remote(msg, dst.at[my_range], sem, (me + step * parts) & (DEVS - 1)).start()
        dst[my_range] = msg[...]

    big = 256

    def products(recv, no, first, last):
        def step(blk, carry):
            rows = pl.ds(pl.multiple_of(blk * big, big), big)
            acc_ref[rows] = apply(mask_ref[rows], recv, no)
            return carry

        lax.fori_loop(first // big, last // big, step, 0)

    arrived(recv0.at[most], row_sem0)
    piled = big // quarters
    if more:
        widen = unfold_hot(big, piled)
        for blk in range(plan.low // big):
            full = dot(widen, recv0[blk * big:(blk + 1) * big, half:]).astype(BF16)
            for c in range(chunks):
                top_ref[blk * piled:(blk + 1) * piled, c * LANES:(c + 1) * LANES] = full[c * piled:(c + 1) * piled]
    tail_msg0[:, :half] = apply(tail_hot, recv0, 0)[:1]
    tail_msg0[:, half:] = facts
    send_tail(tail_msg0, tail_all0, tail_sem0)
    products(recv0, 0, 0, plan.low)
    arrived(recv1.at[most], row_sem1)
    tail_msg1[...] = apply(tail_hot, recv1, 1)[:1]
    send_tail(tail_msg1, tail_all1, tail_sem1)
    tails0 = tail_all0.at[pl.ds(0, plan.ranges - 1)]
    tails1 = tail_all1.at[pl.ds(0, plan.ranges - 1)]
    arrived(tails0, tail_sem0)

    fact = [along_lanes(jnp.where(lane_one == no, tail_all0[:, 0, half:], 0.0)) for no in range(5)]
    range_no = iota((plan.ranges, 1), 0)
    before = range_no < my_range
    same_first = (fact[0] == first[0]) & (fact[1] == first[1])
    same_last = (fact[2] == first[0]) & (fact[3] == first[1])
    stop = before & ((fact[4] > 0.0) | jnp.logical_not(same_first))
    last_stop = jnp.max(jnp.where(stop, range_no, -1), axis=0, keepdims=True)
    linked = before & ((range_no > last_stop) | ((range_no == last_stop) & same_last))

    def carried(tails):
        return along_sublanes(jnp.where(linked, tails[:, 0, :half], 0.0))

    def closed(rows, carry_in):
        return (acc_ref[rows] + jnp.where(bcol_ref[rows][:, :1] == NEG, carry_in, 0.0)).astype(BF16)

    def finish(tails, sums):
        carry_in = carried(tails)

        def step(blk, carry):
            rows = pl.ds(pl.multiple_of(blk * big, big), big)
            sums[rows, :half] = closed(rows, carry_in)
            return carry

        lax.fori_loop(0, plan.low // big, step, 0)

    def send_back(src, dst, sem):
        for dev in others:
            remote(src.at[at16(dev)], dst.at[my_part, at16(my_range)], sem, dev).start()
        dst[my_part, at16(my_range)] = src[at16(me)]

    def finish_top(tails, no):
        top_done[:, no * half:(no + 1) * half] = closed(pl.ds(plan.low, plan.top), carried(tails))

    finish(tail_all0, sums0)
    send_back(sums0, ret0, ret_sem0)

    if more:
        products(recv0, 0, plan.low, plan.need)
        finish_top(tail_all0, 0)
    products(recv1, 1, 0, plan.need)
    arrived(tails1, tail_sem1)
    finish(tail_all1, sums1)
    if more:
        finish_top(tail_all1, 1)
        narrow = fold_hot(big, piled)
        for blk in range(plan.top // piled):
            pile = stack(top_done[blk * piled:(blk + 1) * piled], chunks)
            sums1[blk * big:(blk + 1) * big, half:] = dot(narrow, pile).astype(BF16)
    send_back(sums1, ret1, ret_sem1)

    hot_low_ref[...] = hot(low_col == iota((1, plan.low_out), 1).astype(F32))
    if more:
        fold_ref[...] = unfold_hot(plan.low_out, plan.top_out)
        hot_top_ref[...] = hot(top_col == iota((1, plan.top_out), 1).astype(F32))

    arrived(recv1.at[most], ret_sem0)
    if not more:
        for part in range(parts):
            start = part * cols
            pay_ref[:, start:start + half] = dot(hot_low_ref[...], ret0[part]).astype(BF16)
    else:
        for part in range(parts):
            back_ref[:, part * half:(part + 1) * half] = dot(hot_low_ref[...], ret0[part])
    arrived(recv0.at[most], ret_sem1)
    results = []
    if more:
        piles = jnp.concatenate([ret1[part, :, half:] for part in range(parts)], axis=1)
        piles = dot(fold_ref[...], piles).astype(BF16)
    for part in range(parts):
        start = part * cols
        rows = dot(hot_low_ref[...], ret1[part, :, :half])
        if more:
            top_rows = jnp.concatenate([piles[c * plan.top_out:(c + 1) * plan.top_out, part * LANES:(part + 1) * LANES]
                                        for c in range(chunks)], axis=1)
            top_rows = dot(hot_top_ref[...], top_rows)
            rows = rows + top_rows[:, half:]
            pay_ref[:, start:start + half] = (back_ref[:, part * half:(part + 1) * half] + top_rows[:, :half]).astype(BF16)
        pay_ref[:, start + half:start + cols] = rows.astype(BF16)
        here = pl.ds(start, cols)
        copy = pltpu.make_async_copy(pay_ref.at[:, here], out_hbm.at[:, here], out_sem.at[part])
        copy.start()
        results.append(copy)

    for copy in results:
        copy.wait()

    for like in (samp_all.at[rest], meta_all.at[rest], recv0.at[most], recv1.at[most], tails0, tails1, recv0.at[most],
                 recv1.at[most]):
        left(like)


def run(plan, call_id, keys, segs, payload):
    vmem = pl.BlockSpec(memory_space=pltpu.VMEM)
    shapes = [
        ((ROWS, WIDTH), BF16),
        ((1, LANES), F32),
        ((DEVS, 1, LANES), F32),
        ((plan.low_out, plan.low_out) if plan.more else (BASE, LANES), BF16),
        ((plan.parts, plan.low_out, plan.long), BF16),
        ((plan.parts, plan.low_out, plan.half), BF16),
        ((plan.low, plan.long), BF16),
        ((plan.low, plan.half), BF16),
        ((plan.ranges, 1, LANES), F32),
        ((DEVS, 1, LANES), F32),
        ((plan.need, plan.need), BF16),
        ((plan.need, LANES), F32),
        ((plan.need, LANES), I32),
        ((plan.need, LANES), F32),
        ((plan.need // LANES, 1, LANES), F32),
        ((plan.need // LANES, 1, LANES), I32),
        ((1, plan.half + LANES), F32),
        ((1, plan.half), F32),
        ((plan.ranges, 1, plan.half + LANES), F32),
        ((plan.ranges, 1, plan.half), F32),
        ((max(plan.top, BASE), plan.cols), BF16),
        ((plan.need, plan.half), F32),
        ((max(plan.top, BASE), plan.cols), BF16),
        ((plan.low, plan.half), BF16),
        ((plan.low, plan.long), BF16),
        ((plan.parts, plan.low_out, plan.half), BF16),
        ((plan.parts, plan.low_out, plan.long), BF16),
        ((ROWS, WIDTH // 2) if plan.more else (8, LANES), F32),
        ((ROWS, plan.low_out), BF16),
        ((ROWS, max(plan.top_out, LANES)), BF16),
    ]
    return pl.pallas_call(
        functools.partial(kernel, plan),
        out_shape=(jax.ShapeDtypeStruct((ROWS, WIDTH), BF16), jax.ShapeDtypeStruct((1, 1), F32)),
        in_specs=[vmem, vmem, pl.BlockSpec(memory_space=pl.ANY)],
        out_specs=(pl.BlockSpec(memory_space=pl.ANY), pl.BlockSpec(memory_space=pltpu.SMEM)),
        scratch_shapes=[pltpu.VMEM(*shape) for shape in shapes] + [pltpu.SemaphoreType.DMA] * 10
        + [pltpu.SemaphoreType.DMA((plan.parts,))],
        compiler_params=pltpu.CompilerParams(collective_id=call_id, has_side_effects=True, vmem_limit_bytes=62 << 20),
    )(keys, segs, payload)


def settle_kernel(src_ref, dst_ref, buf, in_sem, out_sem):
    count = in_sem.shape[0]
    tall = ROWS // count
    rows = [pl.ds(no * tall, tall) for no in range(count)]
    into = [pltpu.make_async_copy(src_ref.at[row], buf.at[row], in_sem.at[no]) for no, row in enumerate(rows)]
    out = [pltpu.make_async_copy(buf.at[row], dst_ref.at[row], out_sem.at[no]) for no, row in enumerate(rows)]
    for copy in into:
        copy.start()
    for no in range(count):
        into[no].wait()
        out[no].start()
    for copy in out:
        copy.wait()


def settle(done):
    here = pl.BlockSpec(memory_space=pl.ANY)
    dma = pltpu.SemaphoreType.DMA((4,))
    return pl.pallas_call(settle_kernel, out_shape=jax.ShapeDtypeStruct((ROWS, WIDTH), BF16), in_specs=[here],
                          out_specs=here, scratch_shapes=[pltpu.VMEM((ROWS, WIDTH), BF16), dma, dma])(done)


def solution(mesh):
    def per_device(sort_keys, seg_ids, payload):
        args = (sort_keys.reshape(1, ROWS), seg_ids.reshape(1, ROWS), payload)
        out, flag = run(NARROW, 0, *args)
        return settle(lax.cond(flag[0, 0] > 0.0, lambda done: run(FULL, 1, *args)[0], lambda done: done, out))

    row_spec = P(('batch', 'group'))
    mat_spec = P(('batch', 'group'), None)
    return jax.shard_map(per_device, mesh=mesh, in_specs=(row_spec, row_spec, mat_spec),
                         out_specs=mat_spec, check_vma=False)
```

```python
import functools

import jax
import jax.numpy as jnp
from jax import lax
from jax.experimental import pallas as pl
from jax.experimental.pallas import tpu as pltpu
from jax.sharding import PartitionSpec as P

F32 = jnp.float32
BF16 = jnp.bfloat16
I32 = jnp.int32
NEG = float('-inf')
POS = float('inf')
MESH = pl.DeviceIdType.MESH

DEVS = 128
ROWS = 512
WIDTH = 2048
LANES = 128
BASE = 16
MORE = 4
FLAG = LANES - 1
TALL = 256
RING = 4


class Plan:
    def __init__(self, parts, more, stride):
        self.parts, self.more, self.stride = parts, more, stride
        self.shift = parts.bit_length() - 1
        self.ranges = DEVS // parts
        self.per = ROWS // stride
        self.share = LANES // self.per
        self.cols = WIDTH // parts
        self.half = self.cols // 2
        self.chunks = self.cols // LANES
        self.full = BASE + more
        self.extra = LANES if more else 0
        self.long = self.half + self.extra
        self.low = DEVS * BASE
        self.top = DEVS * more
        self.need = self.low + self.top
        self.low_out = self.ranges * BASE
        self.top_out = self.ranges * more


NARROW = Plan(4, MORE, BASE)
FULL = Plan(2, 0, 4)


def iota(shape, dim):
    return lax.broadcasted_iota(I32, shape, dim)


def ones_where(hit):
    return jnp.where(hit, 1.0, 0.0)


def hot(hit):
    return ones_where(hit).astype(BF16)


def dot(left, right):
    return jnp.dot(left, right, preferred_element_type=F32)


def along_sublanes(vals):
    return jnp.sum(vals, axis=0, keepdims=True)


def along_lanes(vals):
    return jnp.sum(vals, axis=1, keepdims=True)


def fold(to, groups):
    return ((to & (BASE - 1)) >> 2) * groups + (to >> 4) * MORE + (to & (MORE - 1))


def fold_hot(size, groups):
    return hot(fold(iota((size, 1), 0), groups) == iota((1, size), 1))


def unfold_hot(size, groups):
    return hot(iota((size, 1), 0) == fold(iota((1, size), 1), groups))


def stack(rows, chunks):
    return jnp.concatenate([rows[:, c * LANES:(c + 1) * LANES] for c in range(chunks)], axis=0)


def place(me, step):
    core, x, y, z = me & 1, (me >> 1) & (RING - 1), (me >> 3) & (RING - 1), me >> 5
    return (core + step) & 1, ((x + step) & (RING - 1)) << 1, ((y + step) & (RING - 1)) << 3, ((z + step) & (RING - 1)) << 5


def other_devices(me):
    places = [place(me, step) for step in range(RING)]
    found, starts = [], []

    def add(along_x, along_y, along_z, flip):
        found.append(places[along_z % RING][3] + places[along_y % RING][2] + places[along_x][1] + places[flip][0])

    for near in (True, False):
        for flip in range(2):
            starts.append(len(found))
            for along_z in range(RING):
                for along_y in range(RING):
                    if near:
                        add(1, along_y, along_z, flip)
                        add(3, along_y + 2, along_z + 2, flip)
                    else:
                        add(2, along_y + 2, along_z + 2, flip)
                        if along_y or along_z or flip:
                            add(0, along_y, along_z, flip)
    return found, starts


def kernel(plan, keys_ref, segs_ref, pay_hbm, out_hbm, flag_ref, pay_ref, samp_msg, samp_all, fold_ref, packed0, packed1,
           recv0, recv1, meta_msg, meta_all, mask_ref, kcol_ref, scol_ref, bcol_ref, krow_ref, srow_ref, tail_msg0,
           tail_msg1, tail_all0, tail_all1, top_ref, acc_ref, top_done, sums0, sums1, sums_top, ret0, ret1, ret_top, back_ref, hot_low_ref,
           hot_top_ref, pay_sem, send_sem, samp_sem, meta_sem, row_sem0, row_sem1, tail_sem0, tail_sem1, ret_sem0,
           ret_sem1, lines_sem, out_sem):
    parts, more, cols, half, chunks = plan.parts, plan.more, plan.cols, plan.half, plan.chunks
    me = lax.axis_index('group')
    my_range = me >> plan.shift
    my_part = me & (parts - 1)
    barrier = pltpu.get_barrier_semaphore()
    others, starts = other_devices(me)
    rest = pl.ds(0, DEVS - 1)
    most = pl.ds(0, plan.low - BASE)

    def remote(src, dst, recv_sem, dev):
        return pltpu.make_async_remote_copy(src_ref=src, dst_ref=dst, send_sem=send_sem, recv_sem=recv_sem,
                                            device_id={'group': dev}, device_id_type=MESH)

    def arrived(like, sem):
        remote(like, like, sem, others[0]).wait_recv()

    def left(like):
        remote(like, like, ret_sem0, others[0]).wait_send()

    def at16(no):
        return pl.ds(pl.multiple_of(no * BASE, BASE), BASE)

    for dev in others:
        pl.semaphore_signal(barrier, inc=1, device_id={'group': dev}, device_id_type=MESH)
    fetch = pltpu.make_async_copy(pay_hbm, pay_ref, pay_sem)
    fetch.start()

    key_row = keys_ref[...]
    seg_row = segs_ref[...]
    square = (ROWS, ROWS)
    eye = iota(square, 0) == iota(square, 1)

    def to_col(row):
        return along_lanes(jnp.where(eye, jnp.broadcast_to(row, square), 0))

    def to_row(col):
        return along_sublanes(jnp.where(eye, jnp.broadcast_to(col, square), 0))

    key_col = to_col(key_row)
    rank_col = along_lanes(ones_where(key_row < key_col))
    wide = (ROWS, LANES)
    lane_one = iota((1, LANES), 1)
    chosen = ((lane_one - (me & (plan.share - 1)) * plan.per) * plan.stride).astype(F32)
    samp_msg[...] = along_sublanes(jnp.where(rank_col == chosen, jnp.broadcast_to(key_col, wide), 0.0))
    pl.semaphore_wait(barrier, DEVS - 1)

    for dev in others:
        remote(samp_msg, samp_all.at[me], samp_sem, dev).start()
    samp_all[me] = samp_msg[...]
    if more:
        fold_ref[...] = fold_hot(plan.low_out, plan.top_out)
    seg_col = to_col(seg_row)
    arrived(samp_all.at[rest], samp_sem)

    tile = (LANES, LANES)
    counts = []
    for part in range(ROWS // LANES):
        kblk = jnp.broadcast_to(key_col[part * LANES:(part + 1) * LANES], tile)

        def count(step, acc, kblk=kblk):
            for sub in range(8):
                row = (step * 8 + sub) * plan.share
                acc = acc + ones_where(sum(samp_all[row + no] for no in range(plan.share)) <= kblk)
            return acc

        counts.append(along_lanes(lax.fori_loop(0, plan.per // 8, count, jnp.zeros(tile, F32))))
    seen_col = jnp.concatenate(counts, axis=0)
    per_range = DEVS * plan.per // plan.ranges
    range_col = jnp.maximum(jnp.floor((seen_col - (DEVS // 2 + 1)) * (1.0 / per_range)), 0.0)
    range_row = to_row(range_col)
    slot_col = rank_col - along_lanes(ones_where(range_row < range_col))
    low_col = jnp.where(slot_col < BASE, range_col * BASE + slot_col, -1.0)
    low_row = to_row(low_col)
    top_col = jnp.where((slot_col >= BASE) & (slot_col < plan.full), range_col * more + (slot_col - BASE), -1.0)
    spill = ones_where(jnp.max(slot_col, axis=0, keepdims=True) >= plan.full)

    hot_low = hot(low_row == iota((plan.low_out, 1), 0).astype(F32))
    if more:
        hot_top = hot(to_row(top_col) == iota((plan.top_out, 1), 0).astype(F32))
    fetch.wait()
    turns = [others[no] & (parts - 1) for no in starts]

    def pack(part, dst, first):
        start = part * cols + first
        rows = pay_ref[:, pl.ds(pl.multiple_of(start, half), half)]
        dst[part, :, :half] = dot(hot_low, rows).astype(BF16)

    def pack_top(part):
        rows = dot(hot_top, pay_ref[:, pl.ds(pl.multiple_of(part * cols, cols), cols)]).astype(BF16)
        packed0[part, :, half:] = dot(fold_ref[...], stack(rows, chunks)).astype(BF16)

    def pack_first(part):
        pack(part, packed0, 0)
        if more:
            pack_top(part)

    def send_rows(no, src, dst, sem):
        for dev in others[starts[no]:(starts + [DEVS - 1])[no + 1]]:
            remote(src.at[dev & (parts - 1), at16(dev >> plan.shift)], dst.at[at16(me)], sem, dev).start()

    pack_first(turns[0])
    send_rows(0, packed0, recv0, row_sem0)

    lane_val = lane_one // plan.full
    lane_slot = (lane_one % plan.full).astype(F32)
    vals = jnp.where(lane_val == 0, key_col, (seg_col & 65535).astype(F32))
    vals = jnp.where(lane_val == 1, (seg_col >> 16).astype(F32), vals)
    vals = jnp.where((lane_slot == slot_col) & (lane_val < 3), vals, POS)
    range_b = jnp.broadcast_to(range_col, wide)
    for dst in range(plan.ranges):
        meta = jnp.min(jnp.where(range_b == float(dst), vals, POS), axis=0, keepdims=True)
        meta_msg[dst] = jnp.where(lane_one == FLAG, spill, meta)
    for dev in others:
        remote(meta_msg.at[dev >> plan.shift], meta_all.at[me], meta_sem, dev).start()
    meta_all[me] = meta_msg[my_range]
    for no in range(1, len(turns)):
        if no < parts:
            pack_first(turns[no])
        send_rows(no, packed0, recv0, row_sem0)

    for no in range(len(turns)):
        if no < parts:
            pack(turns[no], packed1, half)
        send_rows(no, packed1, recv1, row_sem1)
    recv0[at16(me)] = packed0[my_part, at16(my_range)]
    recv1[at16(me)] = packed1[my_part, at16(my_range)]
    arrived(meta_all.at[rest], meta_sem)

    low_tiles = plan.low // LANES
    tiles = plan.need // LANES
    each = LANES // BASE
    quarters = BASE // MORE
    sub = iota((LANES, 1), 0)
    diag = sub == lane_one

    def read_slots(got, slot):
        found = [along_lanes(jnp.where(lane_one == slot + no * plan.full, got, 0.0)) for no in range(3)]
        live = found[0] < POS
        high, low = [jnp.where(live, val, 0.0).astype(I32) for val in found[1:]]
        return live, found[0], (high << 16) + low

    def keep(step, live, key, seg):
        rows = pl.ds(step * LANES, LANES)
        kcol_ref[rows] = jnp.broadcast_to(jnp.where(live, key, NEG), tile)
        scol_ref[rows] = jnp.broadcast_to(seg, tile)

    def to_lanes(step, spot, key, seg):
        krow_ref[step] = along_sublanes(jnp.where(spot, key, 0.0))
        srow_ref[step] = along_sublanes(jnp.where(spot, seg, 0))

    mixed = []
    for step in range(low_tiles):
        got = meta_all[step * each:(step + 1) * each]
        got = jnp.broadcast_to(got, (each, BASE, LANES)).reshape(tile)
        live, key, seg = read_slots(got, sub & (BASE - 1))
        keep(step, live, key, seg)
        to_lanes(step, diag, key, seg)
        if more:
            turn = step % quarters
            merged = jnp.where(((sub & (BASE - 1)) >> 2) == turn, got, merged if turn else 0.0)
            if turn == quarters - 1:
                mixed.append(merged)
    for no, merged in enumerate(mixed):
        step = low_tiles + no
        _, key, seg = read_slots(merged, BASE + (sub & (MORE - 1)))
        spot = lane_one == (((sub & (BASE - 1)) >> 2) * each + (sub >> 4)) * MORE + (sub & (MORE - 1))
        to_lanes(step, spot, key, seg)
        key = along_lanes(jnp.where(diag, jnp.broadcast_to(krow_ref[step], tile), 0.0))
        seg = along_lanes(jnp.where(diag, jnp.broadcast_to(srow_ref[step], tile), 0))
        keep(step, key < POS, key, seg)
    flags = jnp.max(jnp.where(lane_one == FLAG, meta_all[:, 0, :], 0.0), axis=0, keepdims=True)
    flag_ref[0, 0] = jnp.max(flags)

    def masks(step, carry):
        rows = pl.ds(pl.multiple_of(step * TALL, TALL), TALL)
        kcol = kcol_ref[rows]
        scol = scol_ref[rows]
        best = jnp.full((TALL, LANES), NEG, F32)
        for t in range(tiles):
            best = jnp.maximum(best, jnp.where((krow_ref[t] < kcol) & (srow_ref[t] != scol), krow_ref[t], NEG))
        bound = jnp.broadcast_to(jnp.max(best, axis=1, keepdims=True), best.shape)
        bcol_ref[rows] = bound
        for t in range(tiles):
            mask_ref[rows, t * LANES:(t + 1) * LANES] = hot((krow_ref[t] > bound) & (krow_ref[t] <= kcol))
        return carry

    lax.fori_loop(0, plan.need // TALL, masks, 0)

    krow = [krow_ref[t] for t in range(tiles)]
    srow = [srow_ref[t] for t in range(tiles)]

    def over(items, join, red):
        return red(functools.reduce(join, items), axis=1, keepdims=True)

    key_last = over([jnp.where(k < POS, k, NEG) for k in krow], jnp.maximum, jnp.max)
    key_first = over(krow, jnp.minimum, jnp.min)

    def pick(key):
        seg = over([jnp.where(k == key, s, 0) for k, s in zip(krow, srow)], jnp.add, jnp.sum)
        return seg, [(seg >> 16).astype(F32), (seg & 65535).astype(F32)]

    seg_last, last = pick(key_last)
    _, first = pick(key_first)
    cut = over([jnp.where((k < POS) & (s != seg_last), k, NEG) for k, s in zip(krow, srow)], jnp.maximum, jnp.max)
    tail_hot = jnp.concatenate([ones_where((k > cut) & (k < POS)) for k in krow], axis=1)
    tail_hot = jnp.broadcast_to(tail_hot, (BASE, plan.need)).astype(BF16)
    facts = jnp.zeros((1, LANES), F32)
    for no, val in enumerate(first + last + [ones_where(cut > NEG)]):
        facts = jnp.where(lane_one == no, val, facts)

    def apply(mask, recv, no):
        total = dot(mask[:, :plan.low], recv[:, :half])
        return total + dot(mask[:, plan.low:], top_ref[:, no * half:(no + 1) * half]) if more else total

    def send_tail(msg, dst, sem):
        for step in range(1, plan.ranges):
            remote(msg, dst.at[my_range], sem, (me + step * parts) & (DEVS - 1)).start()
        dst[my_range] = msg[...]

    big = 256

    def products(recv, no, first, last):
        def step(blk, carry):
            rows = pl.ds(pl.multiple_of(blk * big, big), big)
            acc_ref[rows] = apply(mask_ref[rows], recv, no)
            return carry

        lax.fori_loop(first // big, last // big, step, 0)

    arrived(recv0.at[most], row_sem0)
    piled = big // quarters
    if more:
        widen = unfold_hot(big, piled)
        for blk in range(plan.low // big):
            full = dot(widen, recv0[blk * big:(blk + 1) * big, half:]).astype(BF16)
            for c in range(chunks):
                top_ref[blk * piled:(blk + 1) * piled, c * LANES:(c + 1) * LANES] = full[c * piled:(c + 1) * piled]
    tail_msg0[:, :half] = apply(tail_hot, recv0, 0)[:1]
    tail_msg0[:, half:] = facts
    send_tail(tail_msg0, tail_all0, tail_sem0)
    products(recv0, 0, 0, plan.low)
    arrived(recv1.at[most], row_sem1)
    tail_msg1[...] = apply(tail_hot, recv1, 1)[:1]
    send_tail(tail_msg1, tail_all1, tail_sem1)
    tails0 = tail_all0.at[pl.ds(0, plan.ranges - 1)]
    tails1 = tail_all1.at[pl.ds(0, plan.ranges - 1)]
    arrived(tails0, tail_sem0)

    fact = [along_lanes(jnp.where(lane_one == no, tail_all0[:, 0, half:], 0.0)) for no in range(5)]
    range_no = iota((plan.ranges, 1), 0)
    before = range_no < my_range
    same_first = (fact[0] == first[0]) & (fact[1] == first[1])
    same_last = (fact[2] == first[0]) & (fact[3] == first[1])
    stop = before & ((fact[4] > 0.0) | jnp.logical_not(same_first))
    last_stop = jnp.max(jnp.where(stop, range_no, -1), axis=0, keepdims=True)
    linked = before & ((range_no > last_stop) | ((range_no == last_stop) & same_last))

    def carried(tails):
        return along_sublanes(jnp.where(linked, tails[:, 0, :half], 0.0))

    def closed(rows, carry_in):
        return (acc_ref[rows] + jnp.where(bcol_ref[rows][:, :1] == NEG, carry_in, 0.0)).astype(BF16)

    def finish(tails, sums):
        carry_in = carried(tails)

        def step(blk, carry):
            rows = pl.ds(pl.multiple_of(blk * big, big), big)
            sums[rows, :half] = closed(rows, carry_in)
            return carry

        lax.fori_loop(0, plan.low // big, step, 0)

    def send_back(src, dst, sem):
        for dev in others:
            remote(src.at[at16(dev)], dst.at[my_part, at16(my_range)], sem, dev).start()
        dst[my_part, at16(my_range)] = src[at16(me)]

    def finish_top(tails, no):
        top_done[:, no * half:(no + 1) * half] = closed(pl.ds(plan.low, plan.top), carried(tails))

    finish(tail_all0, sums0)
    send_back(sums0, ret0, ret_sem0)

    if more:
        products(recv0, 0, plan.low, plan.need)
        finish_top(tail_all0, 0)
    products(recv1, 1, 0, plan.need)
    arrived(tails1, tail_sem1)
    if more:
        finish_top(tail_all1, 1)
        narrow = fold_hot(big, piled)
        for blk in range(plan.top // piled):
            pile = stack(top_done[blk * piled:(blk + 1) * piled], chunks)
            sums_top[blk * big:(blk + 1) * big] = dot(narrow, pile).astype(BF16)
        send_back(sums_top, ret_top, lines_sem)
    finish(tail_all1, sums1)
    send_back(sums1, ret1, ret_sem1)

    hot_low_ref[...] = hot(low_col == iota((1, plan.low_out), 1).astype(F32))
    if more:
        fold_ref[...] = unfold_hot(plan.low_out, plan.top_out)
        hot_top_ref[...] = hot(top_col == iota((1, plan.top_out), 1).astype(F32))

    arrived(recv1.at[most], ret_sem0)
    if not more:
        for part in range(parts):
            start = part * cols
            pay_ref[:, start:start + half] = dot(hot_low_ref[...], ret0[part]).astype(BF16)
    else:
        for part in range(parts):
            back_ref[:, part * half:(part + 1) * half] = dot(hot_low_ref[...], ret0[part])
    if more:
        arrived(sums_top.at[most], lines_sem)
        piles = jnp.concatenate([ret_top[part] for part in range(parts)], axis=1)
        piles = dot(fold_ref[...], piles).astype(BF16)
        for part in range(parts):
            start = part * cols
            low = slice(part * half, (part + 1) * half)
            top_rows = jnp.concatenate([piles[c * plan.top_out:(c + 1) * plan.top_out, part * LANES:(part + 1) * LANES]
                                        for c in range(chunks)], axis=1)
            top_rows = dot(hot_top_ref[...], top_rows)
            pay_ref[:, start:start + half] = (back_ref[:, low] + top_rows[:, :half]).astype(BF16)
            back_ref[:, low] = top_rows[:, half:]
    arrived(recv1.at[most], ret_sem1)
    results = []
    for part in range(parts):
        start = part * cols
        rows = dot(hot_low_ref[...], ret1[part])
        if more:
            rows = rows + back_ref[:, part * half:(part + 1) * half]
        pay_ref[:, start + half:start + cols] = rows.astype(BF16)
        here = pl.ds(start, cols)
        copy = pltpu.make_async_copy(pay_ref.at[:, here], out_hbm.at[:, here], out_sem.at[part])
        copy.start()
        results.append(copy)

    for copy in results:
        copy.wait()

    for like in (samp_all.at[rest], meta_all.at[rest], recv0.at[most], recv1.at[most], tails0, tails1, recv1.at[most],
                 recv1.at[most]) + ((sums_top.at[most],) if more else ()):
        left(like)


def run(plan, call_id, keys, segs, payload):
    vmem = pl.BlockSpec(memory_space=pltpu.VMEM)
    shapes = [
        ((ROWS, WIDTH), BF16),
        ((1, LANES), F32),
        ((DEVS, 1, LANES), F32),
        ((plan.low_out, plan.low_out) if plan.more else (BASE, LANES), BF16),
        ((plan.parts, plan.low_out, plan.long), BF16),
        ((plan.parts, plan.low_out, plan.half), BF16),
        ((plan.low, plan.long), BF16),
        ((plan.low, plan.half), BF16),
        ((plan.ranges, 1, LANES), F32),
        ((DEVS, 1, LANES), F32),
        ((plan.need, plan.need), BF16),
        ((plan.need, LANES), F32),
        ((plan.need, LANES), I32),
        ((plan.need, LANES), F32),
        ((plan.need // LANES, 1, LANES), F32),
        ((plan.need // LANES, 1, LANES), I32),
        ((1, plan.half + LANES), F32),
        ((1, plan.half), F32),
        ((plan.ranges, 1, plan.half + LANES), F32),
        ((plan.ranges, 1, plan.half), F32),
        ((max(plan.top, BASE), plan.cols), BF16),
        ((plan.need, plan.half), F32),
        ((max(plan.top, BASE), plan.cols), BF16),
        ((plan.low, plan.half), BF16),
        ((plan.low, plan.half), BF16),
        ((plan.low if plan.more else BASE, LANES), BF16),
        ((plan.parts, plan.low_out, plan.half), BF16),
        ((plan.parts, plan.low_out, plan.half), BF16),
        ((plan.parts, plan.low_out if plan.more else BASE, LANES), BF16),
        ((ROWS, WIDTH // 2) if plan.more else (8, LANES), F32),
        ((ROWS, plan.low_out), BF16),
        ((ROWS, max(plan.top_out, LANES)), BF16),
    ]
    return pl.pallas_call(
        functools.partial(kernel, plan),
        out_shape=(jax.ShapeDtypeStruct((ROWS, WIDTH), BF16), jax.ShapeDtypeStruct((1, 1), F32)),
        in_specs=[vmem, vmem, pl.BlockSpec(memory_space=pl.ANY)],
        out_specs=(pl.BlockSpec(memory_space=pl.ANY), pl.BlockSpec(memory_space=pltpu.SMEM)),
        scratch_shapes=[pltpu.VMEM(*shape) for shape in shapes] + [pltpu.SemaphoreType.DMA] * 11
        + [pltpu.SemaphoreType.DMA((plan.parts,))],
        compiler_params=pltpu.CompilerParams(collective_id=call_id, has_side_effects=True, vmem_limit_bytes=62 << 20),
    )(keys, segs, payload)


def settle_kernel(src_ref, dst_ref, buf, in_sem, out_sem):
    count = in_sem.shape[0]
    tall = ROWS // count
    rows = [pl.ds(no * tall, tall) for no in range(count)]
    into = [pltpu.make_async_copy(src_ref.at[row], buf.at[row], in_sem.at[no]) for no, row in enumerate(rows)]
    out = [pltpu.make_async_copy(buf.at[row], dst_ref.at[row], out_sem.at[no]) for no, row in enumerate(rows)]
    for copy in into:
        copy.start()
    for no in range(count):
        into[no].wait()
        out[no].start()
    for copy in out:
        copy.wait()


def settle(done):
    here = pl.BlockSpec(memory_space=pl.ANY)
    dma = pltpu.SemaphoreType.DMA((4,))
    return pl.pallas_call(settle_kernel, out_shape=jax.ShapeDtypeStruct((ROWS, WIDTH), BF16), in_specs=[here],
                          out_specs=here, scratch_shapes=[pltpu.VMEM((ROWS, WIDTH), BF16), dma, dma])(done)


def solution(mesh):
    def per_device(sort_keys, seg_ids, payload):
        args = (sort_keys.reshape(1, ROWS), seg_ids.reshape(1, ROWS), payload)
        out, flag = run(NARROW, 0, *args)
        return settle(lax.cond(flag[0, 0] > 0.0, lambda done: run(FULL, 1, *args)[0], lambda done: done, out))

    row_spec = P(('batch', 'group'))
    mat_spec = P(('batch', 'group'), None)
    return jax.shard_map(per_device, mesh=mesh, in_specs=(row_spec, row_spec, mat_spec),
                         out_specs=mat_spec, check_vma=False)
```
